64 devices in a mesh: dp: 4 (over x, y), sp: 16 (over z, core).
Axes of the slice: x: 2, y: 2, z: 8, core: 2. Of those that a mesh axis runs over, the one named last changes fastest.
The devices are a block of a 4x4x8 slice.
Arguments:
- image_tokens: bfloat16 [128, 256, 1024], P('dp', 'sp'), parts along dimension 0
- ln1_gain: float32 [2, 1024], replicated
- ln1_shift: float32 [2, 1024], replicated
- w_qkv: bfloat16 [2, 1024, 3, 16, 64], replicated
- b_qkv: float32 [2, 3, 16, 64], replicated
- w_out: bfloat16 [2, 16, 64, 1024], replicated
- b_out: float32 [2, 1024], replicated
- ln2_gain: float32 [2, 1024], replicated
- ln2_shift: float32 [2, 1024], replicated
- w_up: bfloat16 [2, 1024, 4096], replicated
- b_up: float32 [2, 4096], replicated
- w_down: bfloat16 [2, 4096, 1024], replicated
- b_down: float32 [2, 1024], replicated
Outputs:
- output: bfloat16 [128, 256, 1024], P('dp', 'sp'), parts along dimension 0
There are 4 independent parts. The reference program is written for one: setup_inputs(seed, part) draws one part's arguments, and reference() takes and returns one part's arrays. A program takes and returns all parts, laid end to end along the dimension named above; an argument that names none is the same for every part.
All inputs are finite; a program needn't handle non-finite values.
Results may differ from the reference program's by a relative error of at most 0.0143029.
Values are sent between devices in bfloat16 or wider.
A program may use at most 768 MiB of HBM per device.

```python
import jax
import jax.numpy as jnp
from jax import lax

IMAGES = 32
SEQ_LEN = 256
WIDTH = 1024
HEADS = 16
HEAD_DIM = 64
MLP_DIM = 4096
LAYERS = 2
LN_EPS = 1e-6


def layer_norm(tokens, ln_gain, ln_shift):
    values = tokens.astype(jnp.float32)
    mean_val = jnp.mean(values, axis=-1, keepdims=True)
    centred = values - mean_val
    var_val = jnp.mean(centred * centred, axis=-1, keepdims=True)
    return (centred * lax.rsqrt(var_val + LN_EPS) * ln_gain + ln_shift).astype(jnp.bfloat16)


def one_head(head_inputs):
    q_head, k_head, v_head = head_inputs
    score_scale = q_head.shape[-1] ** -0.5
    scores = jnp.einsum('bqe,bke->bqk', q_head.astype(jnp.float32), k_head.astype(jnp.float32)) * score_scale
    row_peak = jnp.max(scores, axis=-1, keepdims=True)
    prob_vals = jnp.exp(scores - row_peak)
    row_total = jnp.sum(prob_vals, axis=-1, keepdims=True)
    mixed_vals = jnp.einsum('bqk,bke->bqe', prob_vals.astype(jnp.bfloat16).astype(jnp.float32), v_head.astype(jnp.float32))
    return (mixed_vals / row_total).astype(jnp.bfloat16)


def encoder_layer(hidden, layer_params):
    (ln1_gain, ln1_shift, w_qkv, b_qkv, w_out, b_out, ln2_gain, ln2_shift, w_up, b_up, w_down, b_down) = layer_params
    normed = layer_norm(hidden, ln1_gain, ln1_shift)
    qkv_all = jnp.einsum('bsd,dthe->bsthe', normed.astype(jnp.float32), w_qkv.astype(jnp.float32)) + b_qkv
    per_head = jnp.moveaxis(qkv_all.astype(jnp.bfloat16), 3, 0)
    heads_out = lax.map(one_head, (per_head[:, :, :, 0], per_head[:, :, :, 1], per_head[:, :, :, 2]))
    attn_proj = jnp.einsum('hbse,hed->bsd', heads_out.astype(jnp.float32), w_out.astype(jnp.float32)) + b_out
    mid_state = (hidden.astype(jnp.float32) + attn_proj).astype(jnp.bfloat16)
    normed_two = layer_norm(mid_state, ln2_gain, ln2_shift)
    up_proj = jnp.einsum('bsd,df->bsf', normed_two.astype(jnp.float32), w_up.astype(jnp.float32)) + b_up
    active = jax.nn.gelu(up_proj, approximate=True).astype(jnp.bfloat16)
    down_proj = jnp.einsum('bsf,fd->bsd', active.astype(jnp.float32), w_down.astype(jnp.float32)) + b_down
    return (mid_state.astype(jnp.float32) + down_proj).astype(jnp.bfloat16)


def setup_inputs(seed: int = 0, part: int = 0) -> dict:
    part_key = jax.random.fold_in(jax.random.key(seed), part)
    key_pattern, key_noise = jax.random.split(part_key, 2)
    period = SEQ_LEN // 8
    half_width = WIDTH // 2
    pattern = jax.random.normal(key_pattern, (IMAGES, period, half_width), jnp.float32)
    repeated = jnp.tile(pattern, (1, SEQ_LEN // period, 1))
    noise_part = jax.random.normal(key_noise, (IMAGES, SEQ_LEN, WIDTH - half_width), jnp.float32)
    image_tokens = jnp.concatenate([repeated, noise_part], axis=-1).astype(jnp.bfloat16)
    key_set = jax.random.split(jax.random.key(seed + 1), 14)
    row_scale = jnp.where(jnp.arange(WIDTH) < half_width, 1.0, 0.2)[:, None, None]
    head_shape = (LAYERS, WIDTH, HEADS, HEAD_DIM)
    w_query = 2.0 * WIDTH ** -0.5 * row_scale * jax.random.normal(key_set[0], head_shape, jnp.float32)
    w_key = w_query + 0.1 * WIDTH ** -0.5 * jax.random.normal(key_set[1], head_shape, jnp.float32)
    w_value = WIDTH ** -0.5 * jax.random.normal(key_set[2], head_shape, jnp.float32)
    w_qkv = jnp.stack([w_query, w_key, w_value], axis=2).astype(jnp.bfloat16)
    b_qkv = 0.3 * jax.random.normal(key_set[3], (LAYERS, 3, HEADS, HEAD_DIM), jnp.float32)
    w_out = (1.5 * WIDTH ** -0.5 * jax.random.normal(key_set[4], (LAYERS, HEADS, HEAD_DIM, WIDTH), jnp.float32)).astype(jnp.bfloat16)
    b_out = 0.3 * jax.random.normal(key_set[5], (LAYERS, WIDTH), jnp.float32)
    ln1_gain = 1.0 + 0.2 * jax.random.normal(key_set[6], (LAYERS, WIDTH), jnp.float32)
    ln1_shift = 0.3 * jax.random.normal(key_set[7], (LAYERS, WIDTH), jnp.float32)
    ln2_gain = 1.0 + 0.2 * jax.random.normal(key_set[8], (LAYERS, WIDTH), jnp.float32)
    ln2_shift = 0.3 * jax.random.normal(key_set[9], (LAYERS, WIDTH), jnp.float32)
    w_up = (WIDTH ** -0.5 * jax.random.normal(key_set[10], (LAYERS, WIDTH, MLP_DIM), jnp.float32)).astype(jnp.bfloat16)
    b_up = 0.3 * jax.random.normal(key_set[11], (LAYERS, MLP_DIM), jnp.float32)
    w_down = (0.5 * MLP_DIM ** -0.5 * jax.random.normal(key_set[12], (LAYERS, MLP_DIM, WIDTH), jnp.float32)).astype(jnp.bfloat16)
    b_down = 0.3 * jax.random.normal(key_set[13], (LAYERS, WIDTH), jnp.float32)
    return {'image_tokens': image_tokens, 'ln1_gain': ln1_gain, 'ln1_shift': ln1_shift, 'w_qkv': w_qkv, 'b_qkv': b_qkv, 'w_out': w_out, 'b_out': b_out, 'ln2_gain': ln2_gain, 'ln2_shift': ln2_shift, 'w_up': w_up, 'b_up': b_up, 'w_down': w_down, 'b_down': b_down}


def reference(image_tokens, ln1_gain, ln1_shift, w_qkv, b_qkv, w_out, b_out, ln2_gain, ln2_shift, w_up, b_up, w_down, b_down):
    stacked = (ln1_gain, ln1_shift, w_qkv, b_qkv, w_out, b_out, ln2_gain, ln2_shift, w_up, b_up, w_down, b_down)

    def layer_body(hidden, layer_params):
        return encoder_layer(hidden, layer_params), None

    return lax.scan(layer_body, image_tokens, stacked)[0]
```

```python
import jax
import jax.numpy as jnp
from jax import lax
from jax.sharding import PartitionSpec as P

LN_EPS = 1e-6


def layer_norm(tokens, ln_gain, ln_shift):
    values = tokens.astype(jnp.float32)
    mean_val = jnp.mean(values, axis=-1, keepdims=True)
    centred = values - mean_val
    var_val = jnp.mean(centred * centred, axis=-1, keepdims=True)
    return (centred * lax.rsqrt(var_val + LN_EPS) * ln_gain + ln_shift).astype(jnp.bfloat16)


def attend(q_part, k_part, v_part):
    score_scale = q_part.shape[-1] ** -0.5
    scores = jnp.einsum('bqhe,bkhe->bhqk', q_part, k_part, preferred_element_type=jnp.float32) * score_scale
    row_peak = jnp.max(scores, axis=-1, keepdims=True)
    prob_vals = jnp.exp(scores - row_peak)
    row_total = jnp.sum(prob_vals, axis=-1, keepdims=True)
    mixed_vals = jnp.einsum('bhqk,bkhe->bqhe', prob_vals.astype(jnp.bfloat16), v_part, preferred_element_type=jnp.float32)
    return (mixed_vals / jnp.swapaxes(row_total, 1, 2)).astype(jnp.bfloat16)


def mlp_block(mid_state, ln2_gain, ln2_shift, w_up, b_up, w_down, b_down):
    normed = layer_norm(mid_state, ln2_gain, ln2_shift)
    up_proj = jnp.einsum('bsd,df->bsf', normed, w_up, preferred_element_type=jnp.float32) + b_up
    active = jax.nn.gelu(up_proj, approximate=True).astype(jnp.bfloat16)
    down_proj = jnp.einsum('bsf,fd->bsd', active, w_down, preferred_element_type=jnp.float32) + b_down
    return (mid_state.astype(jnp.float32) + down_proj).astype(jnp.bfloat16)


def solution(mesh):
    token_spec = P('dp', 'sp', None)

    def device_step(image_tokens, ln1_gain, ln1_shift, w_qkv, b_qkv, w_out, b_out, ln2_gain, ln2_shift, w_up, b_up, w_down, b_down):
        hidden = lax.all_to_all(image_tokens, 'sp', 0, 1, tiled=True)
        for layer_idx in range(w_qkv.shape[0]):
            normed = layer_norm(hidden, ln1_gain[layer_idx], ln1_shift[layer_idx])
            qkv = (jnp.einsum('bsd,dthe->bsthe', normed, w_qkv[layer_idx], preferred_element_type=jnp.float32) + b_qkv[layer_idx]).astype(jnp.bfloat16)
            attn = attend(qkv[:, :, 0], qkv[:, :, 1], qkv[:, :, 2])
            attn_proj = jnp.einsum('bshe,hed->bsd', attn, w_out[layer_idx], preferred_element_type=jnp.float32) + b_out[layer_idx]
            mid_state = (hidden.astype(jnp.float32) + attn_proj).astype(jnp.bfloat16)
            hidden = mlp_block(mid_state, ln2_gain[layer_idx], ln2_shift[layer_idx], w_up[layer_idx], b_up[layer_idx], w_down[layer_idx], b_down[layer_idx])
        return lax.all_to_all(hidden, 'sp', 1, 0, tiled=True)

    return jax.shard_map(device_step, mesh=mesh, in_specs=(token_spec,) + (P(),) * 12, out_specs=token_spec, check_vma=False)
```

```python
import functools
import math

import jax
import jax.numpy as jnp
from jax import lax
from jax.experimental import pallas as pl
from jax.experimental.pallas import tpu as pltpu
from jax.sharding import PartitionSpec as P

LN_EPS = 1e-6
MESH = pl.DeviceIdType.MESH
BF = jnp.bfloat16
F32 = jnp.float32
NT = (((1,), (1,)), ((), ()))


def norm_rows(src, dst, gain, shift, rows):
    total = src.shape[0]
    width = src.shape[1]
    for start in range(0, total, rows):
        values = src[pl.ds(start, rows), :].astype(F32)
        mean_val = jnp.sum(values, axis=-1, keepdims=True) * (1.0 / width)
        centred = values - mean_val
        var_val = jnp.sum(centred * centred, axis=-1, keepdims=True) * (1.0 / width)
        dst[pl.ds(start, rows), :] = (centred * lax.rsqrt(var_val + LN_EPS) * gain + shift).astype(BF)


def gelu(x):
    c0 = math.sqrt(2.0 / math.pi)
    c1 = c0 * 0.044715
    return 0.5 * x * (1.0 + jnp.tanh(x * (c0 + c1 * (x * x))))


def kernel(peers, x_ref, g1_hbm, s1_hbm, wqkv_hbm, bqkv_hbm, wout_hbm, bout_hbm, g2_hbm, s2_hbm, wup_hbm, bup_hbm, wdown_hbm, bdown_hbm,
           out_ref,
           hid, wqkv, wout, wup, wdown, g1, s1, bqkv, bout, g2, s2, bup, bdown,
           normed, q_t, v_t, keys, mixed, active,
           w_sem, p_sem, in_send, in_recv, out_send, out_recv):
    images = hid.shape[0]
    block = x_ref.shape[1]
    layers, heads, head_dim = bqkv.shape[0], bqkv.shape[2], bqkv.shape[3]
    tokens, width = hid.shape[1], hid.shape[2]
    mlp_dim = wup.shape[2]
    me = lax.axis_index('sp')

    params = [pltpu.make_async_copy(src, dst, p_sem.at[i]) for i, (src, dst) in enumerate((
        (g1_hbm, g1), (s1_hbm, s1), (bqkv_hbm, bqkv), (bout_hbm, bout), (g2_hbm, g2), (s2_hbm, s2), (bup_hbm, bup), (bdown_hbm, bdown)))]

    def weight_copies(layer):
        return [pltpu.make_async_copy(src.at[layer], dst.at[layer], w_sem.at[layer, i]) for i, (src, dst) in enumerate((
            (wqkv_hbm, wqkv), (wout_hbm, wout), (wup_hbm, wup), (wdown_hbm, wdown)))]

    barrier = pltpu.get_barrier_semaphore()
    for step in range(1, peers):
        pl.semaphore_signal(barrier, inc=1, device_id={'sp': lax.rem(me + step, peers)}, device_id_type=MESH)
    for copy in params:
        copy.start()
    for copy in weight_copies(0):
        copy.start()
    pl.semaphore_wait(barrier, peers - 1)

    order = sorted(range(1, peers), key=lambda s: -min(s // 2, (peers - s) // 2))
    my_rows = pl.ds(pl.multiple_of(me * block, block), block)
    for image in range(images):
        for step in order:
            peer = lax.rem(me + step, peers)
            pltpu.make_async_remote_copy(
                src_ref=x_ref.at[peer * images + image], dst_ref=hid.at[image, my_rows, :],
                send_sem=in_send, recv_sem=in_recv.at[image],
                device_id={'sp': peer}, device_id_type=MESH).start()
        pltpu.make_async_copy(x_ref.at[me * images + image], hid.at[image, my_rows, :], in_recv.at[image]).start()
    for layer in range(1, layers):
        for copy in weight_copies(layer):
            copy.start()
    for copy in params:
        copy.wait()

    def body(step_idx, carry):
        image = step_idx // layers
        layer = lax.rem(step_idx, layers)
        state = hid.at[image]

        def weight_wait(i):
            @pl.when(image == 0)
            def _():
                weight_copies(layer)[i].wait()

        @pl.when(layer == 0)
        def _():
            pltpu.make_async_copy(state, state, in_recv.at[image]).wait()

        row = pl.ds(layer, 1)
        norm_rows(state, normed, g1[row, :], s1[row, :], 32)
        weight_wait(0)

        for slot, dst in ((0, q_t), (2, v_t)):
            bias = bqkv[layer, slot].T
            for start in range(0, width, 512):
                part = lax.dot_general(wqkv[layer, pl.ds(slot * width + start, 512), :], normed[...], NT, preferred_element_type=F32)
                for off in range(0, 512, head_dim):
                    head = (start + off) // head_dim
                    dst[pl.ds(start + off, head_dim), :] = (part[off:off + head_dim] + bias[:, head:head + 1]).astype(BF)
        for start in range(0, width, 512):
            part = lax.dot_general(normed[...], wqkv[layer, pl.ds(width + start, 512), :], NT, preferred_element_type=F32)
            bias = jnp.concatenate([bqkv[layer, 1, pl.ds((start + off) // head_dim, 1), :] for off in range(0, 512, head_dim)], axis=-1)
            keys[:, pl.ds(start, 512)] = (part + bias).astype(BF)

        scale = head_dim ** -0.5 / math.log(2.0)
        zeros = jnp.zeros((head_dim, tokens), BF)
        for pair in range(0, heads, 2):
            cols = pl.ds(pair * head_dim, 2 * head_dim)
            outs = []
            for head in (pair, pair + 1):
                q_head = q_t[pl.ds(head * head_dim, head_dim), :]
                rhs = jnp.concatenate([q_head, zeros] if head == pair else [zeros, q_head], axis=0)
                scores = jnp.dot(keys[:, cols], rhs, preferred_element_type=F32)
                peak = jnp.max(scores, axis=0, keepdims=True)
                prob = jnp.exp2((scores - peak) * scale)
                total = jnp.sum(prob, axis=0, keepdims=True)
                mix = jnp.dot(v_t[pl.ds(head * head_dim, head_dim), :], prob.astype(BF), preferred_element_type=F32)
                outs.append(mix * (1.0 / total))
            mixed[:, cols] = jnp.concatenate(outs, axis=0).T.astype(BF)

        weight_wait(1)
        for start in range(0, width, 512):
            cols = pl.ds(start, 512)
            part = jnp.dot(mixed[...], wout[layer, :, cols], preferred_element_type=F32) + bout[row, cols]
            state[:, cols] = (state[:, cols].astype(F32) + part).astype(BF)

        norm_rows(state, normed, g2[row, :], s2[row, :], 32)
        weight_wait(2)
        for start in range(0, mlp_dim, 512):
            cols = pl.ds(start, 512)
            part = jnp.dot(normed[...], wup[layer, :, cols], preferred_element_type=F32) + bup[row, cols]
            active[:, cols] = gelu(part).astype(BF)
        weight_wait(3)
        for start in range(0, width, 512):
            cols = pl.ds(start, 512)
            part = jnp.dot(active[...], wdown[layer, :, cols], preferred_element_type=F32) + bdown[row, cols]
            state[:, cols] = (state[:, cols].astype(F32) + part).astype(BF)

        @pl.when(layer == layers - 1)
        def _():
            for step in order:
                peer = lax.rem(me + step, peers)
                pltpu.make_async_remote_copy(
                    src_ref=hid.at[image, pl.ds(pl.multiple_of(peer * block, block), block), :],
                    dst_ref=out_ref.at[me * images + image],
                    send_sem=out_send, recv_sem=out_recv,
                    device_id={'sp': peer}, device_id_type=MESH).start()
            pltpu.make_async_copy(hid.at[image, my_rows, :], out_ref.at[me * images + image], out_recv).start()
        return carry

    lax.fori_loop(0, images * layers, body, 0)

    sent = x_ref.at[pl.ds(0, (peers - 1) * images)]
    pltpu.make_async_copy(sent, sent, in_send).wait()
    pltpu.make_async_copy(sent, sent, out_send).wait()
    pltpu.make_async_copy(out_ref, out_ref, out_recv).wait()


def solution(mesh):
    token_spec = P('dp', 'sp', None)
    peers = mesh.shape['sp']

    def device_step(image_tokens, ln1_gain, ln1_shift, w_qkv, b_qkv, w_out, b_out, ln2_gain, ln2_shift, w_up, b_up, w_down, b_down):
        total_images, block, width = image_tokens.shape
        layers, _, _, heads, head_dim = w_qkv.shape
        mlp_dim = w_up.shape[-1]
        images = total_images // peers
        tokens = block * peers
        inner = heads * head_dim
        w_qkv_t = jnp.transpose(w_qkv, (0, 2, 3, 4, 1)).reshape(layers, 3 * inner, width)
        w_out_m = w_out.reshape(layers, inner, width)
        args = (image_tokens, ln1_gain, ln1_shift, w_qkv_t, b_qkv, w_out_m, b_out, ln2_gain, ln2_shift, w_up, b_up, w_down, b_down)
        small = lambda a: pltpu.VMEM(a.shape, a.dtype)
        return pl.pallas_call(
            functools.partial(kernel, peers),
            out_shape=jax.ShapeDtypeStruct(image_tokens.shape, image_tokens.dtype),
            in_specs=[pl.BlockSpec(memory_space=pl.ANY)] * len(args),
            out_specs=pl.BlockSpec(memory_space=pl.ANY),
            scratch_shapes=[
                pltpu.VMEM((images, tokens, width), BF),
                small(w_qkv_t), small(w_out_m), small(w_up), small(w_down),
                small(ln1_gain), small(ln1_shift), small(b_qkv), small(b_out), small(ln2_gain), small(ln2_shift), small(b_up), small(b_down),
                pltpu.VMEM((tokens, width), BF),
                pltpu.VMEM((inner, tokens), BF),
                pltpu.VMEM((inner, tokens), BF),
                pltpu.VMEM((tokens, inner), BF),
                pltpu.VMEM((tokens, inner), BF),
                pltpu.VMEM((tokens, mlp_dim), BF),
                pltpu.SemaphoreType.DMA((layers, 4)),
                pltpu.SemaphoreType.DMA((8,)),
                pltpu.SemaphoreType.DMA,
                pltpu.SemaphoreType.DMA((images,)),
                pltpu.SemaphoreType.DMA,
                pltpu.SemaphoreType.DMA,
            ],
            compiler_params=pltpu.CompilerParams(collective_id=0, has_side_effects=True, vmem_limit_bytes=67_000_000),
        )(*args)

    return jax.shard_map(device_step, mesh=mesh, in_specs=(token_spec,) + (P(),) * 12, out_specs=token_spec, check_vma=False)
```

```python
import functools
import math

import jax
import jax.numpy as jnp
from jax import lax
from jax.experimental import pallas as pl
from jax.experimental.pallas import tpu as pltpu
from jax.sharding import PartitionSpec as P

LN_EPS = 1e-6
MESH = pl.DeviceIdType.MESH
BF = jnp.bfloat16
F32 = jnp.float32
NT = (((1,), (1,)), ((), ()))


def norm_rows(src, dst, gain, shift, rows):
    total = src.shape[0]
    width = src.shape[1]
    for start in range(0, total, rows):
        values = src[pl.ds(start, rows), :].astype(F32)
        mean_val = jnp.sum(values, axis=-1, keepdims=True) * (1.0 / width)
        centred = values - mean_val
        var_val = jnp.sum(centred * centred, axis=-1, keepdims=True) * (1.0 / width)
        dst[pl.ds(start, rows), :] = (centred * lax.rsqrt(var_val + LN_EPS) * gain + shift).astype(BF)


def gelu(x):
    c0 = math.sqrt(2.0 / math.pi)
    c1 = c0 * 0.044715
    return 0.5 * x * (1.0 + jnp.tanh(x * (c0 + c1 * (x * x))))


def kernel(peers, x_ref, g1_hbm, s1_hbm, wqkv_hbm, bqkv_hbm, wout_hbm, bout_hbm, g2_hbm, s2_hbm, wup_hbm, bup_hbm, wdown_hbm, bdown_hbm,
           out_ref,
           hid, wqkv, wout, wup, wdown, g1, s1, bqkv, bout, g2, s2, bup, bdown,
           normed, q_t, v_t, keys, mixed, active,
           w_sem, p_sem, in_send, in_recv, out_send, out_recv):
    images = hid.shape[0]
    block = x_ref.shape[1]
    layers, heads, head_dim = bqkv.shape[0], bqkv.shape[2], bqkv.shape[3]
    tokens, width = hid.shape[1], hid.shape[2]
    mlp_dim = wup.shape[2]
    me = lax.axis_index('sp')

    params = [pltpu.make_async_copy(src, dst, p_sem.at[i]) for i, (src, dst) in enumerate((
        (g1_hbm, g1), (s1_hbm, s1), (bqkv_hbm, bqkv), (bout_hbm, bout), (g2_hbm, g2), (s2_hbm, s2), (bup_hbm, bup), (bdown_hbm, bdown)))]

    def weight_copies(layer):
        return [pltpu.make_async_copy(src.at[layer], dst.at[layer], w_sem.at[layer, i]) for i, (src, dst) in enumerate((
            (wqkv_hbm, wqkv), (wout_hbm, wout), (wup_hbm, wup), (wdown_hbm, wdown)))]

    barrier = pltpu.get_barrier_semaphore()
    for step in range(1, peers):
        pl.semaphore_signal(barrier, inc=1, device_id={'sp': lax.rem(me + step, peers)}, device_id_type=MESH)
    for copy in params:
        copy.start()
    for copy in weight_copies(0):
        copy.start()
    pl.semaphore_wait(barrier, peers - 1)

    order = sorted(range(1, peers), key=lambda s: -min(s // 2, (peers - s) // 2))
    my_rows = pl.ds(pl.multiple_of(me * block, block), block)
    def send_in(image):
        for step in order:
            peer = lax.rem(me + step, peers)
            pltpu.make_async_remote_copy(
                src_ref=x_ref.at[peer * images + image], dst_ref=hid.at[image, my_rows, :],
                send_sem=in_send, recv_sem=in_recv.at[image],
                device_id={'sp': peer}, device_id_type=MESH).start()
        pltpu.make_async_copy(x_ref.at[me * images + image], hid.at[image, my_rows, :], in_recv.at[image]).start()

    send_in(0)
    for layer in range(1, layers):
        for copy in weight_copies(layer):
            copy.start()
    for copy in params:
        copy.wait()

    def body(step_idx, carry):
        image = step_idx // layers
        layer = lax.rem(step_idx, layers)
        state = hid.at[image]

        def weight_wait(i):
            @pl.when(image == 0)
            def _():
                weight_copies(layer)[i].wait()

        @pl.when(layer == 0)
        def _():
            pltpu.make_async_copy(state, state, in_recv.at[image]).wait()

            @pl.when(image < images - 1)
            def _():
                send_in(image + 1)

        row = pl.ds(layer, 1)
        norm_rows(state, normed, g1[row, :], s1[row, :], 32)
        weight_wait(0)

        for slot, dst in ((0, q_t), (2, v_t)):
            bias = bqkv[layer, slot].T
            for start in range(0, width, 512):
                part = lax.dot_general(wqkv[layer, pl.ds(slot * width + start, 512), :], normed[...], NT, preferred_element_type=F32)
                for off in range(0, 512, head_dim):
                    head = (start + off) // head_dim
                    dst[pl.ds(start + off, head_dim), :] = (part[off:off + head_dim] + bias[:, head:head + 1]).astype(BF)
        for start in range(0, width, 512):
            part = lax.dot_general(normed[...], wqkv[layer, pl.ds(width + start, 512), :], NT, preferred_element_type=F32)
            bias = jnp.concatenate([bqkv[layer, 1, pl.ds((start + off) // head_dim, 1), :] for off in range(0, 512, head_dim)], axis=-1)
            keys[:, pl.ds(start, 512)] = (part + bias).astype(BF)

        scale = head_dim ** -0.5 / math.log(2.0)
        zeros = jnp.zeros((head_dim, tokens), BF)
        for pair in range(0, heads, 2):
            cols = pl.ds(pair * head_dim, 2 * head_dim)
            outs = []
            for head in (pair, pair + 1):
                q_head = q_t[pl.ds(head * head_dim, head_dim), :]
                rhs = jnp.concatenate([q_head, zeros] if head == pair else [zeros, q_head], axis=0)
                scores = jnp.dot(keys[:, cols], rhs, preferred_element_type=F32)
                peak = jnp.max(scores, axis=0, keepdims=True)
                prob = jnp.exp2((scores - peak) * scale)
                total = jnp.sum(prob, axis=0, keepdims=True)
                mix = jnp.dot(v_t[pl.ds(head * head_dim, head_dim), :], prob.astype(BF), preferred_element_type=F32)
                outs.append(mix * (1.0 / total))
            mixed[:, cols] = jnp.concatenate(outs, axis=0).T.astype(BF)

        weight_wait(1)
        for start in range(0, width, 512):
            cols = pl.ds(start, 512)
            part = jnp.dot(mixed[...], wout[layer, :, cols], preferred_element_type=F32) + bout[row, cols]
            state[:, cols] = (state[:, cols].astype(F32) + part).astype(BF)

        norm_rows(state, normed, g2[row, :], s2[row, :], 32)
        weight_wait(2)
        for start in range(0, mlp_dim, 512):
            cols = pl.ds(start, 512)
            part = jnp.dot(normed[...], wup[layer, :, cols], preferred_element_type=F32) + bup[row, cols]
            active[:, cols] = gelu(part).astype(BF)
        weight_wait(3)
        for start in range(0, width, 512):
            cols = pl.ds(start, 512)
            part = jnp.dot(active[...], wdown[layer, :, cols], preferred_element_type=F32) + bdown[row, cols]
            state[:, cols] = (state[:, cols].astype(F32) + part).astype(BF)

        @pl.when(layer == layers - 1)
        def _():
            for step in order:
                peer = lax.rem(me + step, peers)
                pltpu.make_async_remote_copy(
                    src_ref=hid.at[image, pl.ds(pl.multiple_of(peer * block, block), block), :],
                    dst_ref=out_ref.at[me * images + image],
                    send_sem=out_send, recv_sem=out_recv,
                    device_id={'sp': peer}, device_id_type=MESH).start()
            pltpu.make_async_copy(hid.at[image, my_rows, :], out_ref.at[me * images + image], out_recv).start()
        return carry

    lax.fori_loop(0, images * layers, body, 0)

    sent = x_ref.at[pl.ds(0, (peers - 1) * images)]
    pltpu.make_async_copy(sent, sent, in_send).wait()
    pltpu.make_async_copy(sent, sent, out_send).wait()
    pltpu.make_async_copy(out_ref, out_ref, out_recv).wait()


def solution(mesh):
    token_spec = P('dp', 'sp', None)
    peers = mesh.shape['sp']

    def device_step(image_tokens, ln1_gain, ln1_shift, w_qkv, b_qkv, w_out, b_out, ln2_gain, ln2_shift, w_up, b_up, w_down, b_down):
        total_images, block, width = image_tokens.shape
        layers, _, _, heads, head_dim = w_qkv.shape
        mlp_dim = w_up.shape[-1]
        images = total_images // peers
        tokens = block * peers
        inner = heads * head_dim
        w_qkv_t = jnp.transpose(w_qkv, (0, 2, 3, 4, 1)).reshape(layers, 3 * inner, width)
        w_out_m = w_out.reshape(layers, inner, width)
        args = (image_tokens, ln1_gain, ln1_shift, w_qkv_t, b_qkv, w_out_m, b_out, ln2_gain, ln2_shift, w_up, b_up, w_down, b_down)
        small = lambda a: pltpu.VMEM(a.shape, a.dtype)
        return pl.pallas_call(
            functools.partial(kernel, peers),
            out_shape=jax.ShapeDtypeStruct(image_tokens.shape, image_tokens.dtype),
            in_specs=[pl.BlockSpec(memory_space=pl.ANY)] * len(args),
            out_specs=pl.BlockSpec(memory_space=pl.ANY),
            scratch_shapes=[
                pltpu.VMEM((images, tokens, width), BF),
                small(w_qkv_t), small(w_out_m), small(w_up), small(w_down),
                small(ln1_gain), small(ln1_shift), small(b_qkv), small(b_out), small(ln2_gain), small(ln2_shift), small(b_up), small(b_down),
                pltpu.VMEM((tokens, width), BF),
                pltpu.VMEM((inner, tokens), BF),
                pltpu.VMEM((inner, tokens), BF),
                pltpu.VMEM((tokens, inner), BF),
                pltpu.VMEM((tokens, inner), BF),
                pltpu.VMEM((tokens, mlp_dim), BF),
                pltpu.SemaphoreType.DMA((layers, 4)),
                pltpu.SemaphoreType.DMA((8,)),
                pltpu.SemaphoreType.DMA,
                pltpu.SemaphoreType.DMA((images,)),
                pltpu.SemaphoreType.DMA,
                pltpu.SemaphoreType.DMA,
            ],
            compiler_params=pltpu.CompilerParams(collective_id=0, has_side_effects=True, vmem_limit_bytes=67_000_000),
        )(*args)

    return jax.shard_map(device_step, mesh=mesh, in_specs=(token_spec,) + (P(),) * 12, out_specs=token_spec, check_vma=False)
```

```python
import functools
import math

import jax
import jax.numpy as jnp
from jax import lax
from jax.experimental import pallas as pl
from jax.experimental.pallas import tpu as pltpu
from jax.sharding import PartitionSpec as P

LN_EPS = 1e-6
MESH = pl.DeviceIdType.MESH
BF = jnp.bfloat16
F32 = jnp.float32
NT = (((1,), (1,)), ((), ()))


def norm_rows(src, dst, gain, shift, rows):
    total = src.shape[0]
    width = src.shape[1]
    for start in range(0, total, rows):
        values = src[pl.ds(start, rows), :].astype(F32)
        mean_val = jnp.sum(values, axis=-1, keepdims=True) * (1.0 / width)
        centred = values - mean_val
        var_val = jnp.sum(centred * centred, axis=-1, keepdims=True) * (1.0 / width)
        dst[pl.ds(start, rows), :] = (centred * lax.rsqrt(var_val + LN_EPS) * gain + shift).astype(BF)


def gelu(x):
    c0 = math.sqrt(2.0 / math.pi)
    c1 = c0 * 0.044715
    return 0.5 * x * (1.0 + jnp.tanh(x * (c0 + c1 * (x * x))))


def kernel(peers, x_ref, g1_hbm, s1_hbm, wqkv_hbm, bqkv_hbm, wout_hbm, bout_hbm, g2_hbm, s2_hbm, wup_hbm, bup_hbm, wdown_hbm, bdown_hbm,
           out_ref,
           hid, wqkv, wout, wup, wdown, g1, s1, bqkv, bout, g2, s2, bup, bdown,
           normed, q_t, v_t, keys, mixed, active, scores, probs, peaks, totals, mixed_t,
           w_sem, p_sem, in_send, in_recv, out_send, out_recv):
    images = hid.shape[0]
    block = x_ref.shape[1]
    layers, heads, head_dim = bqkv.shape[0], bqkv.shape[2], bqkv.shape[3]
    tokens, width = hid.shape[1], hid.shape[2]
    mlp_dim = wup.shape[2]
    me = lax.axis_index('sp')

    params = [pltpu.make_async_copy(src, dst, p_sem.at[i]) for i, (src, dst) in enumerate((
        (g1_hbm, g1), (s1_hbm, s1), (bqkv_hbm, bqkv), (bout_hbm, bout), (g2_hbm, g2), (s2_hbm, s2), (bup_hbm, bup), (bdown_hbm, bdown)))]

    def weight_copies(layer):
        return [pltpu.make_async_copy(src.at[layer], dst.at[layer], w_sem.at[layer, i]) for i, (src, dst) in enumerate((
            (wqkv_hbm, wqkv), (wout_hbm, wout), (wup_hbm, wup), (wdown_hbm, wdown)))]

    barrier = pltpu.get_barrier_semaphore()
    for step in range(1, peers):
        pl.semaphore_signal(barrier, inc=1, device_id={'sp': lax.rem(me + step, peers)}, device_id_type=MESH)
    for copy in params:
        copy.start()
    for copy in weight_copies(0):
        copy.start()
    pl.semaphore_wait(barrier, peers - 1)

    order = sorted(range(1, peers), key=lambda s: -min(s // 2, (peers - s) // 2))
    my_rows = pl.ds(pl.multiple_of(me * block, block), block)
    def send_in(image):
        for step in order:
            peer = lax.rem(me + step, peers)
            pltpu.make_async_remote_copy(
                src_ref=x_ref.at[peer * images + image], dst_ref=hid.at[image, my_rows, :],
                send_sem=in_send, recv_sem=in_recv.at[image],
                device_id={'sp': peer}, device_id_type=MESH).start()
        pltpu.make_async_copy(x_ref.at[me * images + image], hid.at[image, my_rows, :], in_recv.at[image]).start()

    send_in(0)
    for layer in range(1, layers):
        for copy in weight_copies(layer):
            copy.start()
    for copy in params:
        copy.wait()

    def body(step_idx, carry):
        image = step_idx // layers
        layer = lax.rem(step_idx, layers)
        state = hid.at[image]

        def weight_wait(i):
            @pl.when(image == 0)
            def _():
                weight_copies(layer)[i].wait()

        @pl.when(layer == 0)
        def _():
            pltpu.make_async_copy(state, state, in_recv.at[image]).wait()

            @pl.when(image < images - 1)
            def _():
                send_in(image + 1)

        row = pl.ds(layer, 1)
        norm_rows(state, normed, g1[row, :], s1[row, :], 32)
        weight_wait(0)

        for slot, dst in ((0, q_t), (2, v_t)):
            bias = bqkv[layer, slot].T
            for start in range(0, width, 512):
                part = lax.dot_general(wqkv[layer, pl.ds(slot * width + start, 512), :], normed[...], NT, preferred_element_type=F32)
                for off in range(0, 512, head_dim):
                    head = (start + off) // head_dim
                    dst[pl.ds(start + off, head_dim), :] = (part[off:off + head_dim] + bias[:, head:head + 1]).astype(BF)
        for start in range(0, width, 512):
            part = lax.dot_general(normed[...], wqkv[layer, pl.ds(width + start, 512), :], NT, preferred_element_type=F32)
            bias = jnp.concatenate([bqkv[layer, 1, pl.ds((start + off) // head_dim, 1), :] for off in range(0, 512, head_dim)], axis=-1)
            keys[:, pl.ds(start, 512)] = (part + bias).astype(BF)

        scale = head_dim ** -0.5 / math.log(2.0)
        zeros = jnp.zeros((head_dim, tokens), BF)

        def score(head):
            pair = head // 2 * 2
            q_head = q_t[pl.ds(head * head_dim, head_dim), :]
            rhs = jnp.concatenate([q_head, zeros] if head == pair else [zeros, q_head], axis=0)
            part = jnp.dot(keys[:, pl.ds(pair * head_dim, 2 * head_dim)], rhs, preferred_element_type=F32)
            scores[head % 4] = part
            peaks[head % 4] = jnp.max(part, axis=0, keepdims=True)

        def soften(head):
            prob = jnp.exp2((scores[head % 4] - peaks[head % 4]) * scale)
            totals[head % 4] = jnp.sum(prob, axis=0, keepdims=True)
            probs[head % 4] = prob.astype(BF)

        def mix(head):
            part = jnp.dot(v_t[pl.ds(head * head_dim, head_dim), :], probs[head % 4], preferred_element_type=F32)
            mixed_t[pl.ds(head * head_dim, head_dim), :] = part * (1.0 / totals[head % 4])

        for step in range(0, heads + 4, 2):
            for head in (step, step + 1):
                if head < heads:
                    score(head)
            for head in (step - 2, step - 1):
                if 0 <= head < heads:
                    soften(head)
            for head in (step - 4, step - 3):
                if 0 <= head < heads:
                    mix(head)
            if step >= 4:
                cols = pl.ds((step - 4) * head_dim, 2 * head_dim)
                mixed[:, cols] = mixed_t[cols, :].T.astype(BF)

        weight_wait(1)
        for start in range(0, width, 512):
            cols = pl.ds(start, 512)
            part = jnp.dot(mixed[...], wout[layer, :, cols], preferred_element_type=F32) + bout[row, cols]
            state[:, cols] = (state[:, cols].astype(F32) + part).astype(BF)

        norm_rows(state, normed, g2[row, :], s2[row, :], 32)
        weight_wait(2)
        for start in range(0, mlp_dim, 512):
            cols = pl.ds(start, 512)
            part = jnp.dot(normed[...], wup[layer, :, cols], preferred_element_type=F32) + bup[row, cols]
            active[:, cols] = gelu(part).astype(BF)
        weight_wait(3)
        for start in range(0, width, 512):
            cols = pl.ds(start, 512)
            part = jnp.dot(active[...], wdown[layer, :, cols], preferred_element_type=F32) + bdown[row, cols]
            state[:, cols] = (state[:, cols].astype(F32) + part).astype(BF)

        @pl.when(layer == layers - 1)
        def _():
            for step in order:
                peer = lax.rem(me + step, peers)
                pltpu.make_async_remote_copy(
                    src_ref=hid.at[image, pl.ds(pl.multiple_of(peer * block, block), block), :],
                    dst_ref=out_ref.at[me * images + image],
                    send_sem=out_send, recv_sem=out_recv,
                    device_id={'sp': peer}, device_id_type=MESH).start()
            pltpu.make_async_copy(hid.at[image, my_rows, :], out_ref.at[me * images + image], out_recv).start()
        return carry

    lax.fori_loop(0, images * layers, body, 0)

    sent = x_ref.at[pl.ds(0, (peers - 1) * images)]
    pltpu.make_async_copy(sent, sent, in_send).wait()
    pltpu.make_async_copy(sent, sent, out_send).wait()
    pltpu.make_async_copy(out_ref, out_ref, out_recv).wait()


def solution(mesh):
    token_spec = P('dp', 'sp', None)
    peers = mesh.shape['sp']

    def device_step(image_tokens, ln1_gain, ln1_shift, w_qkv, b_qkv, w_out, b_out, ln2_gain, ln2_shift, w_up, b_up, w_down, b_down):
        total_images, block, width = image_tokens.shape
        layers, _, _, heads, head_dim = w_qkv.shape
        mlp_dim = w_up.shape[-1]
        images = total_images // peers
        tokens = block * peers
        inner = heads * head_dim
        w_qkv_t = jnp.transpose(w_qkv, (0, 2, 3, 4, 1)).reshape(layers, 3 * inner, width)
        w_out_m = w_out.reshape(layers, inner, width)
        args = (image_tokens, ln1_gain, ln1_shift, w_qkv_t, b_qkv, w_out_m, b_out, ln2_gain, ln2_shift, w_up, b_up, w_down, b_down)
        small = lambda a: pltpu.VMEM(a.shape, a.dtype)
        return pl.pallas_call(
            functools.partial(kernel, peers),
            out_shape=jax.ShapeDtypeStruct(image_tokens.shape, image_tokens.dtype),
            in_specs=[pl.BlockSpec(memory_space=pl.ANY)] * len(args),
            out_specs=pl.BlockSpec(memory_space=pl.ANY),
            scratch_shapes=[
                pltpu.VMEM((images, tokens, width), BF),
                small(w_qkv_t), small(w_out_m), small(w_up), small(w_down),
                small(ln1_gain), small(ln1_shift), small(b_qkv), small(b_out), small(ln2_gain), small(ln2_shift), small(b_up), small(b_down),
                pltpu.VMEM((tokens, width), BF),
                pltpu.VMEM((inner, tokens), BF),
                pltpu.VMEM((inner, tokens), BF),
                pltpu.VMEM((tokens, inner), BF),
                pltpu.VMEM((tokens, inner), BF),
                pltpu.VMEM((tokens, mlp_dim), BF),
                pltpu.VMEM((4, tokens, tokens), F32),
                pltpu.VMEM((4, tokens, tokens), BF),
                pltpu.VMEM((4, 1, tokens), F32),
                pltpu.VMEM((4, 1, tokens), F32),
                pltpu.VMEM((inner, tokens), F32),
                pltpu.SemaphoreType.DMA((layers, 4)),
                pltpu.SemaphoreType.DMA((8,)),
                pltpu.SemaphoreType.DMA,
                pltpu.SemaphoreType.DMA((images,)),
                pltpu.SemaphoreType.DMA,
                pltpu.SemaphoreType.DMA,
            ],
            compiler_params=pltpu.CompilerParams(collective_id=0, has_side_effects=True, vmem_limit_bytes=67_000_000),
        )(*args)

    return jax.shard_map(device_step, mesh=mesh, in_specs=(token_spec,) + (P(),) * 12, out_specs=token_spec, check_vma=False)
```

```python
import functools
import math

import jax
import jax.numpy as jnp
from jax import lax
from jax.experimental import pallas as pl
from jax.experimental.pallas import tpu as pltpu
from jax.sharding import PartitionSpec as P

LN_EPS = 1e-6
MESH = pl.DeviceIdType.MESH
BF = jnp.bfloat16
F32 = jnp.float32
NT = (((1,), (1,)), ((), ()))


def norm_rows(src, dst, gain, shift, rows):
    total = src.shape[0]
    width = src.shape[1]
    for start in range(0, total, rows):
        values = src[pl.ds(start, rows), :].astype(F32)
        mean_val = jnp.sum(values, axis=-1, keepdims=True) * (1.0 / width)
        centred = values - mean_val
        var_val = jnp.sum(centred * centred, axis=-1, keepdims=True) * (1.0 / width)
        dst[pl.ds(start, rows), :] = (centred * lax.rsqrt(var_val + LN_EPS) * gain + shift).astype(BF)


def gelu(x):
    c0 = math.sqrt(2.0 / math.pi)
    c1 = c0 * 0.044715
    return 0.5 * x * (1.0 + jnp.tanh(x * (c0 + c1 * (x * x))))


def kernel(peers, x_ref, g1_hbm, s1_hbm, wqkv_hbm, bqkv_hbm, wout_hbm, bout_hbm, g2_hbm, s2_hbm, wup_hbm, bup_hbm, wdown_hbm, bdown_hbm,
           out_ref,
           hid, wqkv, wout, wup, wdown, g1, s1, bqkv, bout, g2, s2, bup, bdown,
           normed, q_t, v_t, keys, mixed, active, scores, probs, peaks, totals, mixed_t,
           w_sem, p_sem, in_send, in_recv, out_send, out_recv):
    images = hid.shape[0]
    block = x_ref.shape[1]
    layers, heads, head_dim = bqkv.shape[0], bqkv.shape[2], bqkv.shape[3]
    tokens, width = hid.shape[1], hid.shape[2]
    mlp_dim = wup.shape[2]
    me = lax.axis_index('sp')

    params = [pltpu.make_async_copy(src, dst, p_sem.at[i]) for i, (src, dst) in enumerate((
        (g1_hbm, g1), (s1_hbm, s1), (bqkv_hbm, bqkv), (bout_hbm, bout), (g2_hbm, g2), (s2_hbm, s2), (bup_hbm, bup), (bdown_hbm, bdown)))]

    def weight_copies(layer):
        return [pltpu.make_async_copy(src.at[layer], dst.at[layer], w_sem.at[layer, i]) for i, (src, dst) in enumerate((
            (wqkv_hbm, wqkv), (wout_hbm, wout), (wup_hbm, wup), (wdown_hbm, wdown)))]

    barrier = pltpu.get_barrier_semaphore()
    for step in range(1, peers):
        pl.semaphore_signal(barrier, inc=1, device_id={'sp': lax.rem(me + step, peers)}, device_id_type=MESH)
    for copy in params:
        copy.start()
    for copy in weight_copies(0):
        copy.start()
    pl.semaphore_wait(barrier, peers - 1)

    order = sorted(range(1, peers), key=lambda s: -min(s // 2, (peers - s) // 2))
    my_rows = pl.ds(pl.multiple_of(me * block, block), block)
    def send_in(image):
        for step in order:
            peer = lax.rem(me + step, peers)
            pltpu.make_async_remote_copy(
                src_ref=x_ref.at[peer * images + image], dst_ref=hid.at[image, my_rows, :],
                send_sem=in_send, recv_sem=in_recv.at[image],
                device_id={'sp': peer}, device_id_type=MESH).start()
        pltpu.make_async_copy(x_ref.at[me * images + image], hid.at[image, my_rows, :], in_recv.at[image]).start()

    send_in(0)
    for layer in range(1, layers):
        for copy in weight_copies(layer):
            copy.start()
    for copy in params:
        copy.wait()

    def body(step_idx, carry):
        image = step_idx // layers
        layer = lax.rem(step_idx, layers)
        state = hid.at[image]

        @pl.when(image == 0)
        def _():
            for copy in weight_copies(layer):
                copy.wait()

        @pl.when(layer == 0)
        def _():
            pltpu.make_async_copy(state, state, in_recv.at[image]).wait()

            @pl.when(image < images - 1)
            def _():
                send_in(image + 1)

        row = pl.ds(layer, 1)
        norm_rows(state, normed, g1[row, :], s1[row, :], 32)

        for slot, dst in ((0, q_t), (2, v_t)):
            bias = bqkv[layer, slot].T
            for start in range(0, width, 512):
                part = lax.dot_general(wqkv[layer, pl.ds(slot * width + start, 512), :], normed[...], NT, preferred_element_type=F32)
                for off in range(0, 512, head_dim):
                    head = (start + off) // head_dim
                    dst[pl.ds(start + off, head_dim), :] = (part[off:off + head_dim] + bias[:, head:head + 1]).astype(BF)
        for start in range(0, width, 512):
            part = lax.dot_general(normed[...], wqkv[layer, pl.ds(width + start, 512), :], NT, preferred_element_type=F32)
            bias = jnp.concatenate([bqkv[layer, 1, pl.ds((start + off) // head_dim, 1), :] for off in range(0, 512, head_dim)], axis=-1)
            keys[:, pl.ds(start, 512)] = (part + bias).astype(BF)

        scale = head_dim ** -0.5 / math.log(2.0)
        zeros = jnp.zeros((head_dim, tokens), BF)

        def score(head):
            pair = head // 2 * 2
            q_head = q_t[pl.ds(head * head_dim, head_dim), :]
            rhs = jnp.concatenate([q_head, zeros] if head == pair else [zeros, q_head], axis=0)
            part = jnp.dot(keys[:, pl.ds(pair * head_dim, 2 * head_dim)], rhs, preferred_element_type=F32)
            scores[head % 4] = part
            peaks[head % 4] = jnp.max(part, axis=0, keepdims=True)

        def soften(head):
            prob = jnp.exp2((scores[head % 4] - peaks[head % 4]) * scale)
            totals[head % 4] = jnp.sum(prob, axis=0, keepdims=True)
            probs[head % 4] = prob.astype(BF)

        def mix(head):
            part = jnp.dot(v_t[pl.ds(head * head_dim, head_dim), :], probs[head % 4], preferred_element_type=F32)
            mixed_t[pl.ds(head * head_dim, head_dim), :] = part * (1.0 / totals[head % 4])

        for step in range(0, heads + 4, 2):
            for head in (step, step + 1):
                if head < heads:
                    score(head)
            for head in (step - 2, step - 1):
                if 0 <= head < heads:
                    soften(head)
            for head in (step - 4, step - 3):
                if 0 <= head < heads:
                    mix(head)
            if step >= 4:
                cols = pl.ds((step - 4) * head_dim, 2 * head_dim)
                mixed[:, cols] = mixed_t[cols, :].T.astype(BF)

        for start in range(0, width, 512):
            cols = pl.ds(start, 512)
            part = jnp.dot(mixed[...], wout[layer, :, cols], preferred_element_type=F32) + bout[row, cols]
            state[:, cols] = (state[:, cols].astype(F32) + part).astype(BF)

        norm_rows(state, normed, g2[row, :], s2[row, :], 32)
        for start in range(0, mlp_dim, 512):
            cols = pl.ds(start, 512)
            part = jnp.dot(normed[...], wup[layer, :, cols], preferred_element_type=F32) + bup[row, cols]
            active[:, cols] = gelu(part).astype(BF)
        for start in range(0, width, 512):
            cols = pl.ds(start, 512)
            part = jnp.dot(active[...], wdown[layer, :, cols], preferred_element_type=F32) + bdown[row, cols]
            state[:, cols] = (state[:, cols].astype(F32) + part).astype(BF)

        @pl.when(layer == layers - 1)
        def _():
            for step in order:
                peer = lax.rem(me + step, peers)
                pltpu.make_async_remote_copy(
                    src_ref=hid.at[image, pl.ds(pl.multiple_of(peer * block, block), block), :],
                    dst_ref=out_ref.at[me * images + image],
                    send_sem=out_send, recv_sem=out_recv,
                    device_id={'sp': peer}, device_id_type=MESH).start()
            pltpu.make_async_copy(hid.at[image, my_rows, :], out_ref.at[me * images + image], out_recv).start()
        return carry

    lax.fori_loop(0, images * layers, body, 0)

    sent = x_ref.at[pl.ds(0, (peers - 1) * images)]
    pltpu.make_async_copy(sent, sent, in_send).wait()
    pltpu.make_async_copy(sent, sent, out_send).wait()
    pltpu.make_async_copy(out_ref, out_ref, out_recv).wait()


def solution(mesh):
    token_spec = P('dp', 'sp', None)
    peers = mesh.shape['sp']

    def device_step(image_tokens, ln1_gain, ln1_shift, w_qkv, b_qkv, w_out, b_out, ln2_gain, ln2_shift, w_up, b_up, w_down, b_down):
        total_images, block, width = image_tokens.shape
        layers, _, _, heads, head_dim = w_qkv.shape
        mlp_dim = w_up.shape[-1]
        images = total_images // peers
        tokens = block * peers
        inner = heads * head_dim
        w_qkv_t = jnp.transpose(w_qkv, (0, 2, 3, 4, 1)).reshape(layers, 3 * inner, width)
        w_out_m = w_out.reshape(layers, inner, width)
        args = (image_tokens, ln1_gain, ln1_shift, w_qkv_t, b_qkv, w_out_m, b_out, ln2_gain, ln2_shift, w_up, b_up, w_down, b_down)
        small = lambda a: pltpu.VMEM(a.shape, a.dtype)
        return pl.pallas_call(
            functools.partial(kernel, peers),
            out_shape=jax.ShapeDtypeStruct(image_tokens.shape, image_tokens.dtype),
            in_specs=[pl.BlockSpec(memory_space=pl.ANY)] * len(args),
            out_specs=pl.BlockSpec(memory_space=pl.ANY),
            scratch_shapes=[
                pltpu.VMEM((images, tokens, width), BF),
                small(w_qkv_t), small(w_out_m), small(w_up), small(w_down),
                small(ln1_gain), small(ln1_shift), small(b_qkv), small(b_out), small(ln2_gain), small(ln2_shift), small(b_up), small(b_down),
                pltpu.VMEM((tokens, width), BF),
                pltpu.VMEM((inner, tokens), BF),
                pltpu.VMEM((inner, tokens), BF),
                pltpu.VMEM((tokens, inner), BF),
                pltpu.VMEM((tokens, inner), BF),
                pltpu.VMEM((tokens, mlp_dim), BF),
                pltpu.VMEM((4, tokens, tokens), F32),
                pltpu.VMEM((4, tokens, tokens), BF),
                pltpu.VMEM((4, 1, tokens), F32),
                pltpu.VMEM((4, 1, tokens), F32),
                pltpu.VMEM((inner, tokens), F32),
                pltpu.SemaphoreType.DMA((layers, 4)),
                pltpu.SemaphoreType.DMA((8,)),
                pltpu.SemaphoreType.DMA,
                pltpu.SemaphoreType.DMA((images,)),
                pltpu.SemaphoreType.DMA,
                pltpu.SemaphoreType.DMA,
            ],
            compiler_params=pltpu.CompilerParams(collective_id=0, has_side_effects=True, vmem_limit_bytes=67_000_000),
        )(*args)

    return jax.shard_map(device_step, mesh=mesh, in_specs=(token_spec,) + (P(),) * 12, out_specs=token_spec, check_vma=False)
```

```python
import functools
import math

import jax
import jax.numpy as jnp
from jax import lax
from jax.experimental import pallas as pl
from jax.experimental.pallas import tpu as pltpu
from jax.sharding import PartitionSpec as P

LN_EPS = 1e-6
MESH = pl.DeviceIdType.MESH
BF = jnp.bfloat16
F32 = jnp.float32
NT = (((1,), (1,)), ((), ()))


def norm_rows(src, dst, gain, shift, rows):
    total = src.shape[0]
    width = src.shape[1]
    for start in range(0, total, rows):
        values = src[pl.ds(start, rows), :].astype(F32)
        mean_val = jnp.sum(values, axis=-1, keepdims=True) * (1.0 / width)
        centred = values - mean_val
        var_val = jnp.sum(centred * centred, axis=-1, keepdims=True) * (1.0 / width)
        dst[pl.ds(start, rows), :] = (centred * lax.rsqrt(var_val + LN_EPS) * gain + shift).astype(BF)


def gelu(x):
    c0 = math.sqrt(2.0 / math.pi)
    c1 = c0 * 0.044715
    return 0.5 * x * (1.0 + jnp.tanh(x * (c0 + c1 * (x * x))))


def kernel(peers, x_ref, g1_hbm, s1_hbm, wqkv_hbm, bqkv_hbm, wout_hbm, bout_hbm, g2_hbm, s2_hbm, wup_hbm, bup_hbm, wdown_hbm, bdown_hbm,
           out_ref,
           hid, wqkv, wout, wup, wdown, g1, s1, bqkv, bout, g2, s2, bup, bdown,
           normed, q_t, v_t, keys, mixed, active, scores, probs, peaks, totals, mixed_t,
           ready, w_sem, p_sem, in_send, in_recv, out_send, out_recv):
    images = hid.shape[0]
    block = x_ref.shape[1]
    layers, heads, head_dim = bqkv.shape[0], bqkv.shape[2], bqkv.shape[3]
    tokens, width = hid.shape[1], hid.shape[2]
    mlp_dim = wup.shape[2]
    me = lax.axis_index('sp')

    params = [pltpu.make_async_copy(src, dst, p_sem.at[i]) for i, (src, dst) in enumerate((
        (g1_hbm, g1), (s1_hbm, s1), (bqkv_hbm, bqkv), (bout_hbm, bout), (g2_hbm, g2), (s2_hbm, s2), (bup_hbm, bup), (bdown_hbm, bdown)))]

    def weight_copies(layer):
        return [pltpu.make_async_copy(src.at[layer], dst.at[layer], w_sem.at[layer, i]) for i, (src, dst) in enumerate((
            (wqkv_hbm, wqkv), (wout_hbm, wout), (wup_hbm, wup), (wdown_hbm, wdown)))]

    my_rows = pl.ds(pl.multiple_of(me * block, block), block)

    def send_in(image, peer):
        pltpu.make_async_remote_copy(
            src_ref=x_ref.at[peer * images + image], dst_ref=hid.at[image, my_rows, :],
            send_sem=in_send, recv_sem=in_recv.at[image],
            device_id={'sp': peer}, device_id_type=MESH).start()

    barrier = pltpu.get_barrier_semaphore()

    @pl.loop(me + 1, peers)
    def _(peer):
        pl.semaphore_signal(barrier, inc=1, device_id={'sp': peer}, device_id_type=MESH)

    @pl.when(me > 0)
    def _():
        pl.semaphore_wait(barrier, me)

    @pl.loop(0, me)
    def _(peer):
        pl.semaphore_signal(ready.at[me], inc=1, device_id={'sp': peer}, device_id_type=MESH)

    @pl.loop(0, me)
    def _(peer):
        send_in(0, peer)

    for copy in params:
        copy.start()
    for copy in weight_copies(0):
        copy.start()

    @pl.loop(me + 1, peers)
    def _(peer):
        pl.semaphore_wait(ready.at[peer], 1)
        send_in(0, peer)

    for image in range(images):
        pltpu.make_async_copy(x_ref.at[me * images + image], hid.at[image, my_rows, :], in_recv.at[image]).start()
    for image in range(1, images):
        @pl.loop(0, me)
        def _(peer):
            send_in(image, peer)

        @pl.loop(me + 1, peers)
        def _(peer):
            send_in(image, peer)

    for layer in range(1, layers):
        for copy in weight_copies(layer):
            copy.start()
    for copy in params:
        copy.wait()

    def body(step_idx, carry):
        image = step_idx // layers
        layer = lax.rem(step_idx, layers)
        state = hid.at[image]

        @pl.when(image == 0)
        def _():
            for copy in weight_copies(layer):
                copy.wait()

        @pl.when(layer == 0)
        def _():
            pltpu.make_async_copy(state, state, in_recv.at[image]).wait()

        row = pl.ds(layer, 1)
        norm_rows(state, normed, g1[row, :], s1[row, :], 32)

        for slot, dst in ((0, q_t), (2, v_t)):
            bias = bqkv[layer, slot].T
            for start in range(0, width, 512):
                part = lax.dot_general(wqkv[layer, pl.ds(slot * width + start, 512), :], normed[...], NT, preferred_element_type=F32)
                for off in range(0, 512, head_dim):
                    head = (start + off) // head_dim
                    dst[pl.ds(start + off, head_dim), :] = (part[off:off + head_dim] + bias[:, head:head + 1]).astype(BF)
        for start in range(0, width, 512):
            part = lax.dot_general(normed[...], wqkv[layer, pl.ds(width + start, 512), :], NT, preferred_element_type=F32)
            bias = jnp.concatenate([bqkv[layer, 1, pl.ds((start + off) // head_dim, 1), :] for off in range(0, 512, head_dim)], axis=-1)
            keys[:, pl.ds(start, 512)] = (part + bias).astype(BF)

        scale = head_dim ** -0.5 / math.log(2.0)
        zeros = jnp.zeros((head_dim, tokens), BF)

        def score(head):
            pair = head // 2 * 2
            q_head = q_t[pl.ds(head * head_dim, head_dim), :]
            rhs = jnp.concatenate([q_head, zeros] if head == pair else [zeros, q_head], axis=0)
            part = jnp.dot(keys[:, pl.ds(pair * head_dim, 2 * head_dim)], rhs, preferred_element_type=F32)
            scores[head % 4] = part
            peaks[head % 4] = jnp.max(part, axis=0, keepdims=True)

        def soften(head):
            prob = jnp.exp2((scores[head % 4] - peaks[head % 4]) * scale)
            totals[head % 4] = jnp.sum(prob, axis=0, keepdims=True)
            probs[head % 4] = prob.astype(BF)

        def mix(head):
            part = jnp.dot(v_t[pl.ds(head * head_dim, head_dim), :], probs[head % 4], preferred_element_type=F32)
            mixed_t[pl.ds(head * head_dim, head_dim), :] = part * (1.0 / totals[head % 4])

        for step in range(0, heads + 4, 2):
            for head in (step, step + 1):
                if head < heads:
                    score(head)
            for head in (step - 2, step - 1):
                if 0 <= head < heads:
                    soften(head)
            for head in (step - 4, step - 3):
                if 0 <= head < heads:
                    mix(head)
            if step >= 4:
                cols = pl.ds((step - 4) * head_dim, 2 * head_dim)
                mixed[:, cols] = mixed_t[cols, :].T.astype(BF)

        for start in range(0, width, 512):
            cols = pl.ds(start, 512)
            part = jnp.dot(mixed[...], wout[layer, :, cols], preferred_element_type=F32) + bout[row, cols]
            state[:, cols] = (state[:, cols].astype(F32) + part).astype(BF)

        norm_rows(state, normed, g2[row, :], s2[row, :], 32)
        for start in range(0, mlp_dim, 512):
            cols = pl.ds(start, 512)
            part = jnp.dot(normed[...], wup[layer, :, cols], preferred_element_type=F32) + bup[row, cols]
            active[:, cols] = gelu(part).astype(BF)
        for start in range(0, width, 512):
            cols = pl.ds(start, 512)
            part = jnp.dot(active[...], wdown[layer, :, cols], preferred_element_type=F32) + bdown[row, cols]
            state[:, cols] = (state[:, cols].astype(F32) + part).astype(BF)

        @pl.when(layer == layers - 1)
        def _():
            @pl.loop(1, peers)
            def _(step):
                peer = lax.rem(me + step, peers)
                pltpu.make_async_remote_copy(
                    src_ref=hid.at[image, pl.ds(pl.multiple_of(peer * block, block), block), :],
                    dst_ref=out_ref.at[me * images + image],
                    send_sem=out_send, recv_sem=out_recv,
                    device_id={'sp': peer}, device_id_type=MESH).start()

            pltpu.make_async_copy(hid.at[image, my_rows, :], out_ref.at[me * images + image], out_recv).start()
        return carry

    lax.fori_loop(0, images * layers, body, 0)

    sent = x_ref.at[pl.ds(0, (peers - 1) * images)]
    pltpu.make_async_copy(sent, sent, in_send).wait()
    pltpu.make_async_copy(sent, sent, out_send).wait()
    pltpu.make_async_copy(out_ref, out_ref, out_recv).wait()


def solution(mesh):
    token_spec = P('dp', 'sp', None)
    peers = mesh.shape['sp']

    def device_step(image_tokens, ln1_gain, ln1_shift, w_qkv, b_qkv, w_out, b_out, ln2_gain, ln2_shift, w_up, b_up, w_down, b_down):
        total_images, block, width = image_tokens.shape
        layers, _, _, heads, head_dim = w_qkv.shape
        mlp_dim = w_up.shape[-1]
        images = total_images // peers
        tokens = block * peers
        inner = heads * head_dim
        w_qkv_t = jnp.transpose(w_qkv, (0, 2, 3, 4, 1)).reshape(layers, 3 * inner, width)
        w_out_m = w_out.reshape(layers, inner, width)
        args = (image_tokens, ln1_gain, ln1_shift, w_qkv_t, b_qkv, w_out_m, b_out, ln2_gain, ln2_shift, w_up, b_up, w_down, b_down)
        small = lambda a: pltpu.VMEM(a.shape, a.dtype)
        return pl.pallas_call(
            functools.partial(kernel, peers),
            out_shape=jax.ShapeDtypeStruct(image_tokens.shape, image_tokens.dtype),
            in_specs=[pl.BlockSpec(memory_space=pl.ANY)] * len(args),
            out_specs=pl.BlockSpec(memory_space=pl.ANY),
            scratch_shapes=[
                pltpu.VMEM((images, tokens, width), BF),
                small(w_qkv_t), small(w_out_m), small(w_up), small(w_down),
                small(ln1_gain), small(ln1_shift), small(b_qkv), small(b_out), small(ln2_gain), small(ln2_shift), small(b_up), small(b_down),
                pltpu.VMEM((tokens, width), BF),
                pltpu.VMEM((inner, tokens), BF),
                pltpu.VMEM((inner, tokens), BF),
                pltpu.VMEM((tokens, inner), BF),
                pltpu.VMEM((tokens, inner), BF),
                pltpu.VMEM((tokens, mlp_dim), BF),
                pltpu.VMEM((4, tokens, tokens), F32),
                pltpu.VMEM((4, tokens, tokens), BF),
                pltpu.VMEM((4, 1, tokens), F32),
                pltpu.VMEM((4, 1, tokens), F32),
                pltpu.VMEM((inner, tokens), F32),
                pltpu.SemaphoreType.REGULAR((peers,)),
                pltpu.SemaphoreType.DMA((layers, 4)),
                pltpu.SemaphoreType.DMA((8,)),
                pltpu.SemaphoreType.DMA,
                pltpu.SemaphoreType.DMA((images,)),
                pltpu.SemaphoreType.DMA,
                pltpu.SemaphoreType.DMA,
            ],
            compiler_params=pltpu.CompilerParams(collective_id=0, has_side_effects=True, vmem_limit_bytes=67_000_000),
        )(*args)

    return jax.shard_map(device_step, mesh=mesh, in_specs=(token_spec,) + (P(),) * 12, out_specs=token_spec, check_vma=False)
```

```python
import functools
import math

import jax
import jax.numpy as jnp
from jax import lax
from jax.experimental import pallas as pl
from jax.experimental.pallas import tpu as pltpu
from jax.sharding import PartitionSpec as P

LN_EPS = 1e-6
MESH = pl.DeviceIdType.MESH
BF = jnp.bfloat16
F32 = jnp.float32
NT = (((1,), (1,)), ((), ()))


def norm_rows(src, dst, gain, shift, rows):
    total = src.shape[0]
    width = src.shape[1]
    for start in range(0, total, rows):
        values = src[pl.ds(start, rows), :].astype(F32)
        mean_val = jnp.sum(values, axis=-1, keepdims=True) * (1.0 / width)
        centred = values - mean_val
        var_val = jnp.sum(centred * centred, axis=-1, keepdims=True) * (1.0 / width)
        dst[pl.ds(start, rows), :] = (centred * lax.rsqrt(var_val + LN_EPS) * gain + shift).astype(BF)


def gelu(x):
    c0 = math.sqrt(2.0 / math.pi)
    c1 = c0 * 0.044715
    return 0.5 * x * (1.0 + jnp.tanh(x * (c0 + c1 * (x * x))))


def kernel(peers, x_ref, g1_hbm, s1_hbm, wqkv_hbm, bqkv_hbm, wout_hbm, bout_hbm, g2_hbm, s2_hbm, wup_hbm, bup_hbm, wdown_hbm, bdown_hbm,
           out_ref,
           hid, wqkv, wout, wup, wdown, g1, s1, bqkv, bout, g2, s2, bup, bdown,
           normed, q_t, v_t, keys, mixed, active, scores, probs, peaks, totals, mixed_t,
           ready, w_sem, p_sem, in_send, in_recv, out_send, out_recv):
    images = hid.shape[0]
    block = x_ref.shape[1]
    layers, heads, head_dim = bqkv.shape[0], bqkv.shape[2], bqkv.shape[3]
    tokens, width = hid.shape[1], hid.shape[2]
    mlp_dim = wup.shape[2]
    me = lax.axis_index('sp')

    params = [pltpu.make_async_copy(src, dst, p_sem.at[i]) for i, (src, dst) in enumerate((
        (g1_hbm, g1), (s1_hbm, s1), (bqkv_hbm, bqkv), (bout_hbm, bout), (g2_hbm, g2), (s2_hbm, s2), (bup_hbm, bup), (bdown_hbm, bdown)))]

    def weight_copies(layer):
        return [pltpu.make_async_copy(src.at[layer], dst.at[layer], w_sem.at[layer, i]) for i, (src, dst) in enumerate((
            (wqkv_hbm, wqkv), (wout_hbm, wout), (wup_hbm, wup), (wdown_hbm, wdown)))]

    my_rows = pl.ds(pl.multiple_of(me * block, block), block)

    def send_in(image, peer):
        pltpu.make_async_remote_copy(
            src_ref=x_ref.at[peer * images + image], dst_ref=hid.at[image, my_rows, :],
            send_sem=in_send, recv_sem=in_recv.at[image],
            device_id={'sp': peer}, device_id_type=MESH).start()

    barrier = pltpu.get_barrier_semaphore()

    @pl.loop(me + 1, peers)
    def _(peer):
        pl.semaphore_signal(barrier, inc=1, device_id={'sp': peer}, device_id_type=MESH)

    @pl.when(me > 0)
    def _():
        pl.semaphore_wait(barrier, me)

    @pl.loop(0, me)
    def _(peer):
        pl.semaphore_signal(ready.at[me], inc=1, device_id={'sp': peer}, device_id_type=MESH)

    for core in range(2):
        @pl.loop(0, me)
        def _(peer):
            @pl.when(lax.rem(peer, 2) == core)
            def _():
                send_in(0, peer)

    for copy in params:
        copy.start()
    for copy in weight_copies(0):
        copy.start()

    @pl.loop(me + 1, peers)
    def _(peer):
        pl.semaphore_wait(ready.at[peer], 1)
        send_in(0, peer)

    pltpu.make_async_copy(x_ref.at[me * images], hid.at[0, my_rows, :], in_recv.at[0]).start()
    for layer in range(1, layers):
        for copy in weight_copies(layer):
            copy.start()
    for copy in params:
        copy.wait()

    def body(step_idx, carry):
        image = step_idx // layers
        layer = lax.rem(step_idx, layers)
        state = hid.at[image]

        @pl.when(image == 0)
        def _():
            for copy in weight_copies(layer):
                copy.wait()

        @pl.when(layer == 0)
        def _():
            pltpu.make_async_copy(state, state, in_recv.at[image]).wait()

            @pl.when(image < images - 1)
            def _():
                pltpu.make_async_copy(x_ref.at[me * images + image + 1], hid.at[image + 1, my_rows, :], in_recv.at[image + 1]).start()

                @pl.loop(1, peers)
                def _(step):
                    send_in(image + 1, lax.rem(me + step, peers))

        row = pl.ds(layer, 1)
        norm_rows(state, normed, g1[row, :], s1[row, :], 32)

        for slot, dst in ((0, q_t), (2, v_t)):
            bias = bqkv[layer, slot].T
            for start in range(0, width, 512):
                part = lax.dot_general(wqkv[layer, pl.ds(slot * width + start, 512), :], normed[...], NT, preferred_element_type=F32)
                for off in range(0, 512, head_dim):
                    head = (start + off) // head_dim
                    dst[pl.ds(start + off, head_dim), :] = (part[off:off + head_dim] + bias[:, head:head + 1]).astype(BF)
        for start in range(0, width, 512):
            part = lax.dot_general(normed[...], wqkv[layer, pl.ds(width + start, 512), :], NT, preferred_element_type=F32)
            bias = jnp.concatenate([bqkv[layer, 1, pl.ds((start + off) // head_dim, 1), :] for off in range(0, 512, head_dim)], axis=-1)
            keys[:, pl.ds(start, 512)] = (part + bias).astype(BF)

        scale = head_dim ** -0.5 / math.log(2.0)
        zeros = jnp.zeros((head_dim, tokens), BF)

        def score(head):
            pair = head // 2 * 2
            q_head = q_t[pl.ds(head * head_dim, head_dim), :]
            rhs = jnp.concatenate([q_head, zeros] if head == pair else [zeros, q_head], axis=0)
            part = jnp.dot(keys[:, pl.ds(pair * head_dim, 2 * head_dim)], rhs, preferred_element_type=F32)
            scores[head % 4] = part
            peaks[head % 4] = jnp.max(part, axis=0, keepdims=True)

        def soften(head):
            prob = jnp.exp2((scores[head % 4] - peaks[head % 4]) * scale)
            totals[head % 4] = jnp.sum(prob, axis=0, keepdims=True)
            probs[head % 4] = prob.astype(BF)

        def mix(head):
            part = jnp.dot(v_t[pl.ds(head * head_dim, head_dim), :], probs[head % 4], preferred_element_type=F32)
            mixed_t[pl.ds(head * head_dim, head_dim), :] = part * (1.0 / totals[head % 4])

        for step in range(0, heads + 4, 2):
            for head in (step, step + 1):
                if head < heads:
                    score(head)
            for head in (step - 2, step - 1):
                if 0 <= head < heads:
                    soften(head)
            for head in (step - 4, step - 3):
                if 0 <= head < heads:
                    mix(head)
            if step >= 4:
                cols = pl.ds((step - 4) * head_dim, 2 * head_dim)
                mixed[:, cols] = mixed_t[cols, :].T.astype(BF)

        for start in range(0, width, 512):
            cols = pl.ds(start, 512)
            part = jnp.dot(mixed[...], wout[layer, :, cols], preferred_element_type=F32) + bout[row, cols]
            state[:, cols] = (state[:, cols].astype(F32) + part).astype(BF)

        half = tokens // 2

        def norm_two(first):
            norm_rows(state.at[pl.ds(first, half), :], normed.at[pl.ds(first, half), :], g2[row, :], s2[row, :], 32)

        def widen(first):
            rows = pl.ds(first, half)
            for start in range(0, mlp_dim, 512):
                cols = pl.ds(start, 512)
                part = jnp.dot(normed[rows, :], wup[layer, :, cols], preferred_element_type=F32) + bup[row, cols]
                active[rows, cols] = gelu(part).astype(BF)

        def narrow(first):
            rows = pl.ds(first, half)
            for start in range(0, width, 512):
                cols = pl.ds(start, 512)
                part = jnp.dot(active[rows, :], wdown[layer, :, cols], preferred_element_type=F32) + bdown[row, cols]
                state[rows, cols] = (state[rows, cols].astype(F32) + part).astype(BF)

        def send_out(first):
            @pl.when(layer == layers - 1)
            def _():
                low = first // block
                high = low + half // block
                slot = me * images + image

                @pl.loop(low, high)
                def _(peer):
                    rows = pl.ds(pl.multiple_of(peer * block, block), block)

                    @pl.when(peer != me)
                    def _():
                        pltpu.make_async_remote_copy(
                            src_ref=hid.at[image, rows, :], dst_ref=out_ref.at[slot],
                            send_sem=out_send, recv_sem=out_recv,
                            device_id={'sp': peer}, device_id_type=MESH).start()

                    @pl.when(peer == me)
                    def _():
                        out_ref[slot] = hid[image, rows, :]

        norm_two(0)
        widen(0)
        norm_two(half)
        narrow(0)
        send_out(0)
        widen(half)
        narrow(half)
        send_out(half)
        return carry

    lax.fori_loop(0, images * layers, body, 0)

    sent = x_ref.at[pl.ds(0, (peers - 1) * images)]
    pltpu.make_async_copy(sent, sent, in_send).wait()
    pltpu.make_async_copy(sent, sent, out_send).wait()
    pltpu.make_async_copy(sent, sent, out_recv).wait()


def solution(mesh):
    token_spec = P('dp', 'sp', None)
    peers = mesh.shape['sp']

    def device_step(image_tokens, ln1_gain, ln1_shift, w_qkv, b_qkv, w_out, b_out, ln2_gain, ln2_shift, w_up, b_up, w_down, b_down):
        total_images, block, width = image_tokens.shape
        layers, _, _, heads, head_dim = w_qkv.shape
        mlp_dim = w_up.shape[-1]
        images = total_images // peers
        tokens = block * peers
        inner = heads * head_dim
        w_qkv_t = jnp.transpose(w_qkv, (0, 2, 3, 4, 1)).reshape(layers, 3 * inner, width)
        w_out_m = w_out.reshape(layers, inner, width)
        args = (image_tokens, ln1_gain, ln1_shift, w_qkv_t, b_qkv, w_out_m, b_out, ln2_gain, ln2_shift, w_up, b_up, w_down, b_down)
        small = lambda a: pltpu.VMEM(a.shape, a.dtype)
        return pl.pallas_call(
            functools.partial(kernel, peers),
            out_shape=pltpu.VMEM(image_tokens.shape, image_tokens.dtype),
            in_specs=[pl.BlockSpec(memory_space=pl.ANY)] * len(args),
            out_specs=pl.BlockSpec(memory_space=pltpu.VMEM),
            scratch_shapes=[
                pltpu.VMEM((images, tokens, width), BF),
                small(w_qkv_t), small(w_out_m), small(w_up), small(w_down),
                small(ln1_gain), small(ln1_shift), small(b_qkv), small(b_out), small(ln2_gain), small(ln2_shift), small(b_up), small(b_down),
                pltpu.VMEM((tokens, width), BF),
                pltpu.VMEM((inner, tokens), BF),
                pltpu.VMEM((inner, tokens), BF),
                pltpu.VMEM((tokens, inner), BF),
                pltpu.VMEM((tokens, inner), BF),
                pltpu.VMEM((tokens, mlp_dim), BF),
                pltpu.VMEM((4, tokens, tokens), F32),
                pltpu.VMEM((4, tokens, tokens), BF),
                pltpu.VMEM((4, 1, tokens), F32),
                pltpu.VMEM((4, 1, tokens), F32),
                pltpu.VMEM((inner, tokens), F32),
                pltpu.SemaphoreType.REGULAR((peers,)),
                pltpu.SemaphoreType.DMA((layers, 4)),
                pltpu.SemaphoreType.DMA((8,)),
                pltpu.SemaphoreType.DMA,
                pltpu.SemaphoreType.DMA((images,)),
                pltpu.SemaphoreType.DMA,
                pltpu.SemaphoreType.DMA,
            ],
            compiler_params=pltpu.CompilerParams(collective_id=0, has_side_effects=True, vmem_limit_bytes=65_500_000),
        )(*args)

    return jax.shard_map(device_step, mesh=mesh, in_specs=(token_spec,) + (P(),) * 12, out_specs=token_spec, check_vma=False)
```

```python
import functools
import math

import jax
import jax.numpy as jnp
from jax import lax
from jax.experimental import pallas as pl
from jax.experimental.pallas import tpu as pltpu
from jax.sharding import PartitionSpec as P

LN_EPS = 1e-6
MESH = pl.DeviceIdType.MESH
BF = jnp.bfloat16
F32 = jnp.float32
NT = (((1,), (1,)), ((), ()))


def norm_rows(src, dst, gain, shift, rows):
    total = src.shape[0]
    width = src.shape[1]
    for start in range(0, total, rows):
        values = src[pl.ds(start, rows), :].astype(F32)
        mean_val = jnp.sum(values, axis=-1, keepdims=True) * (1.0 / width)
        centred = values - mean_val
        var_val = jnp.sum(centred * centred, axis=-1, keepdims=True) * (1.0 / width)
        dst[pl.ds(start, rows), :] = (centred * lax.rsqrt(var_val + LN_EPS) * gain + shift).astype(BF)


def gelu(x):
    c0 = math.sqrt(2.0 / math.pi)
    c1 = c0 * 0.044715
    return 0.5 * x * (1.0 + jnp.tanh(x * (c0 + c1 * (x * x))))


def kernel(peers, x_ref, g1_hbm, s1_hbm, wqkv_hbm, bqkv_hbm, wout_hbm, bout_hbm, g2_hbm, s2_hbm, wup_hbm, bup_hbm, wdown_hbm, bdown_hbm,
           out_ref,
           hid, wqkv, wout, wup, wdown, g1, s1, bqkv, bout, g2, s2, bup, bdown,
           normed, q_t, v_t, keys, mixed, active, scores, probs, peaks, totals, mixed_t,
           ready, w_sem, p_sem, in_send, in_recv, out_send, out_recv):
    images = hid.shape[0]
    block = x_ref.shape[1]
    layers, heads, head_dim = bqkv.shape[0], bqkv.shape[2], bqkv.shape[3]
    tokens, width = hid.shape[1], hid.shape[2]
    mlp_dim = wup.shape[2]
    me = lax.axis_index('sp')

    params = [pltpu.make_async_copy(src, dst, p_sem.at[i]) for i, (src, dst) in enumerate((
        (g1_hbm, g1), (s1_hbm, s1), (bqkv_hbm, bqkv), (bout_hbm, bout), (g2_hbm, g2), (s2_hbm, s2), (bup_hbm, bup), (bdown_hbm, bdown)))]

    def weight_copies(layer):
        return [pltpu.make_async_copy(src.at[layer], dst.at[layer], w_sem.at[layer, i]) for i, (src, dst) in enumerate((
            (wqkv_hbm, wqkv), (wout_hbm, wout), (wup_hbm, wup), (wdown_hbm, wdown)))]

    my_rows = pl.ds(pl.multiple_of(me * block, block), block)

    def send_in(image, ask):
        chips = peers // 2
        for core in range(2):
            for parity in range(2):
                @pl.loop(0, chips // 2)
                def _(turn):
                    peer = 4 * lax.rem(me // 4 + turn, chips // 2) + 2 * parity + core

                    if ask:
                        @pl.when(peer > me)
                        def _():
                            pl.semaphore_wait(ready.at[peer], 1)

                    @pl.when(peer != me)
                    def _():
                        pltpu.make_async_remote_copy(
                            src_ref=x_ref.at[peer * images + image], dst_ref=hid.at[image, my_rows, :],
                            send_sem=in_send, recv_sem=in_recv.at[image],
                            device_id={'sp': peer}, device_id_type=MESH).start()
        pltpu.make_async_copy(x_ref.at[me * images + image], hid.at[image, my_rows, :], in_recv.at[image]).start()

    for copy in params:
        copy.start()
    for copy in weight_copies(0):
        copy.start()

    barrier = pltpu.get_barrier_semaphore()

    @pl.loop(me + 1, peers)
    def _(peer):
        pl.semaphore_signal(barrier, inc=1, device_id={'sp': peer}, device_id_type=MESH)

    @pl.when(me > 0)
    def _():
        pl.semaphore_wait(barrier, me)

    @pl.loop(0, me)
    def _(peer):
        pl.semaphore_signal(ready.at[me], inc=1, device_id={'sp': peer}, device_id_type=MESH)

    send_in(0, True)
    for layer in range(1, layers):
        for copy in weight_copies(layer):
            copy.start()
    for copy in params:
        copy.wait()

    def body(step_idx, carry):
        image = step_idx // layers
        layer = lax.rem(step_idx, layers)
        state = hid.at[image]

        @pl.when(image == 0)
        def _():
            for copy in weight_copies(layer):
                copy.wait()

        @pl.when(layer == 0)
        def _():
            pltpu.make_async_copy(state, state, in_recv.at[image]).wait()

        row = pl.ds(layer, 1)
        norm_rows(state, normed, g1[row, :], s1[row, :], 32)

        for slot, dst in ((0, q_t), (2, v_t)):
            bias = bqkv[layer, slot].T
            for start in range(0, width, 512):
                part = lax.dot_general(wqkv[layer, pl.ds(slot * width + start, 512), :], normed[...], NT, preferred_element_type=F32)
                for off in range(0, 512, head_dim):
                    head = (start + off) // head_dim
                    dst[pl.ds(start + off, head_dim), :] = (part[off:off + head_dim] + bias[:, head:head + 1]).astype(BF)
        for start in range(0, width, 512):
            part = lax.dot_general(normed[...], wqkv[layer, pl.ds(width + start, 512), :], NT, preferred_element_type=F32)
            bias = jnp.concatenate([bqkv[layer, 1, pl.ds((start + off) // head_dim, 1), :] for off in range(0, 512, head_dim)], axis=-1)
            keys[:, pl.ds(start, 512)] = (part + bias).astype(BF)

        scale = head_dim ** -0.5 / math.log(2.0)
        zeros = jnp.zeros((head_dim, tokens), BF)

        def score(head):
            pair = head // 2 * 2
            q_head = q_t[pl.ds(head * head_dim, head_dim), :]
            rhs = jnp.concatenate([q_head, zeros] if head == pair else [zeros, q_head], axis=0)
            part = jnp.dot(keys[:, pl.ds(pair * head_dim, 2 * head_dim)], rhs, preferred_element_type=F32)
            scores[head % 4] = part
            peaks[head % 4] = jnp.max(part, axis=0, keepdims=True)

        def soften(head):
            prob = jnp.exp2((scores[head % 4] - peaks[head % 4]) * scale)
            totals[head % 4] = jnp.sum(prob, axis=0, keepdims=True)
            probs[head % 4] = prob.astype(BF)

        def mix(head):
            part = jnp.dot(v_t[pl.ds(head * head_dim, head_dim), :], probs[head % 4], preferred_element_type=F32)
            mixed_t[pl.ds(head * head_dim, head_dim), :] = part * (1.0 / totals[head % 4])

        for step in range(0, heads + 4, 2):
            for head in (step, step + 1):
                if head < heads:
                    score(head)
            for head in (step - 2, step - 1):
                if 0 <= head < heads:
                    soften(head)
            for head in (step - 4, step - 3):
                if 0 <= head < heads:
                    mix(head)
            if step >= 4:
                cols = pl.ds((step - 4) * head_dim, 2 * head_dim)
                mixed[:, cols] = mixed_t[cols, :].T.astype(BF)

        for start in range(0, width, 512):
            cols = pl.ds(start, 512)
            part = jnp.dot(mixed[...], wout[layer, :, cols], preferred_element_type=F32) + bout[row, cols]
            state[:, cols] = (state[:, cols].astype(F32) + part).astype(BF)

        @pl.when(step_idx == 0)
        def _():
            for other in range(1, images):
                send_in(other, False)

        norm_rows(state, normed, g2[row, :], s2[row, :], 32)
        for start in range(0, mlp_dim, 512):
            cols = pl.ds(start, 512)
            part = jnp.dot(normed[...], wup[layer, :, cols], preferred_element_type=F32) + bup[row, cols]
            active[:, cols] = gelu(part).astype(BF)
        for start in range(0, width, 512):
            cols = pl.ds(start, 512)
            part = jnp.dot(active[...], wdown[layer, :, cols], preferred_element_type=F32) + bdown[row, cols]
            state[:, cols] = (state[:, cols].astype(F32) + part).astype(BF)

        @pl.when(layer == layers - 1)
        def _():
            slot = me * images + image

            @pl.loop(0, peers)
            def _(peer):
                rows = pl.ds(pl.multiple_of(peer * block, block), block)

                @pl.when(peer != me)
                def _():
                    pltpu.make_async_remote_copy(
                        src_ref=hid.at[image, rows, :], dst_ref=out_ref.at[slot],
                        send_sem=out_send, recv_sem=out_recv,
                        device_id={'sp': peer}, device_id_type=MESH).start()

                @pl.when(peer == me)
                def _():
                    out_ref[slot] = hid[image, rows, :]

        return carry

    lax.fori_loop(0, images * layers, body, 0)

    sent = x_ref.at[pl.ds(0, (peers - 1) * images)]
    pltpu.make_async_copy(sent, sent, in_send).wait()
    pltpu.make_async_copy(sent, sent, out_send).wait()
    pltpu.make_async_copy(sent, sent, out_recv).wait()


def solution(mesh):
    token_spec = P('dp', 'sp', None)
    peers = mesh.shape['sp']

    def device_step(image_tokens, ln1_gain, ln1_shift, w_qkv, b_qkv, w_out, b_out, ln2_gain, ln2_shift, w_up, b_up, w_down, b_down):
        total_images, block, width = image_tokens.shape
        layers, _, _, heads, head_dim = w_qkv.shape
        mlp_dim = w_up.shape[-1]
        images = total_images // peers
        tokens = block * peers
        inner = heads * head_dim
        w_qkv_t = jnp.transpose(w_qkv, (0, 2, 3, 4, 1)).reshape(layers, 3 * inner, width)
        w_out_m = w_out.reshape(layers, inner, width)
        args = (image_tokens, ln1_gain, ln1_shift, w_qkv_t, b_qkv, w_out_m, b_out, ln2_gain, ln2_shift, w_up, b_up, w_down, b_down)
        small = lambda a: pltpu.VMEM(a.shape, a.dtype)
        return pl.pallas_call(
            functools.partial(kernel, peers),
            out_shape=pltpu.VMEM(image_tokens.shape, image_tokens.dtype),
            in_specs=[pl.BlockSpec(memory_space=pl.ANY)] * len(args),
            out_specs=pl.BlockSpec(memory_space=pltpu.VMEM),
            scratch_shapes=[
                pltpu.VMEM((images, tokens, width), BF),
                small(w_qkv_t), small(w_out_m), small(w_up), small(w_down),
                small(ln1_gain), small(ln1_shift), small(b_qkv), small(b_out), small(ln2_gain), small(ln2_shift), small(b_up), small(b_down),
                pltpu.VMEM((tokens, width), BF),
                pltpu.VMEM((inner, tokens), BF),
                pltpu.VMEM((inner, tokens), BF),
                pltpu.VMEM((tokens, inner), BF),
                pltpu.VMEM((tokens, inner), BF),
                pltpu.VMEM((tokens, mlp_dim), BF),
                pltpu.VMEM((4, tokens, tokens), F32),
                pltpu.VMEM((4, tokens, tokens), BF),
                pltpu.VMEM((4, 1, tokens), F32),
                pltpu.VMEM((4, 1, tokens), F32),
                pltpu.VMEM((inner, tokens), F32),
                pltpu.SemaphoreType.REGULAR((peers,)),
                pltpu.SemaphoreType.DMA((layers, 4)),
                pltpu.SemaphoreType.DMA((8,)),
                pltpu.SemaphoreType.DMA,
                pltpu.SemaphoreType.DMA((images,)),
                pltpu.SemaphoreType.DMA,
                pltpu.SemaphoreType.DMA,
            ],
            compiler_params=pltpu.CompilerParams(collective_id=0, has_side_effects=True, vmem_limit_bytes=65_500_000),
        )(*args)

    return jax.shard_map(device_step, mesh=mesh, in_specs=(token_spec,) + (P(),) * 12, out_specs=token_spec, check_vma=False)
```

```python
import functools
import math

import jax
import jax.numpy as jnp
from jax import lax
from jax.experimental import pallas as pl
from jax.experimental.pallas import tpu as pltpu
from jax.sharding import PartitionSpec as P

LN_EPS = 1e-6
MESH = pl.DeviceIdType.MESH
BF = jnp.bfloat16
F32 = jnp.float32
NT = (((1,), (1,)), ((), ()))


def norm_rows(src, dst, gain, shift, rows):
    total = src.shape[0]
    width = src.shape[1]
    for start in range(0, total, rows):
        values = src[pl.ds(start, rows), :].astype(F32)
        mean_val = jnp.sum(values, axis=-1, keepdims=True) * (1.0 / width)
        centred = values - mean_val
        var_val = jnp.sum(centred * centred, axis=-1, keepdims=True) * (1.0 / width)
        dst[pl.ds(start, rows), :] = (centred * lax.rsqrt(var_val + LN_EPS) * gain + shift).astype(BF)


def gelu(x):
    c0 = math.sqrt(2.0 / math.pi)
    c1 = c0 * 0.044715
    return 0.5 * x * (1.0 + jnp.tanh(x * (c0 + c1 * (x * x))))


def hops(peers, parity):
    chips = peers // 2
    return sorted(range(parity, chips, 2), key=lambda hop: (-min(hop, chips - hop), hop))


def kernel(peers, x_ref, g1_hbm, s1_hbm, wqkv_hbm, bqkv_hbm, wout_hbm, bout_hbm, g2_hbm, s2_hbm, wup_hbm, bup_hbm, wdown_hbm, bdown_hbm,
           out_ref,
           hid, wqkv, wout, wup, wdown, g1, s1, bqkv, bout, g2, s2, bup, bdown,
           normed, q_t, v_t, keys, mixed, active, scores, probs, peaks, totals, mixed_t,
           ready, w_sem, p_sem, in_send, in_recv, out_send, out_recv):
    images = hid.shape[0]
    block = x_ref.shape[1]
    layers, heads, head_dim = bqkv.shape[0], bqkv.shape[2], bqkv.shape[3]
    tokens, width = hid.shape[1], hid.shape[2]
    mlp_dim = wup.shape[2]
    me = lax.axis_index('sp')

    params = [pltpu.make_async_copy(src, dst, p_sem.at[i]) for i, (src, dst) in enumerate((
        (g1_hbm, g1), (s1_hbm, s1), (bqkv_hbm, bqkv), (bout_hbm, bout), (g2_hbm, g2), (s2_hbm, s2), (bup_hbm, bup), (bdown_hbm, bdown)))]

    def weight_copies(layer):
        return [pltpu.make_async_copy(src.at[layer], dst.at[layer], w_sem.at[layer, i]) for i, (src, dst) in enumerate((
            (wqkv_hbm, wqkv), (wout_hbm, wout), (wup_hbm, wup), (wdown_hbm, wdown)))]

    my_rows = pl.ds(pl.multiple_of(me * block, block), block)

    def send_in(image, ask):
        for core in range(2):
            for parity in range(2):
                odd = lax.rem(me // 2 + parity, 2)
                for even_hop, odd_hop in zip(hops(peers, 0), hops(peers, 1)):
                    peer = 2 * lax.rem(me // 2 + even_hop + odd * (odd_hop - even_hop), peers // 2) + core

                    if ask:
                        @pl.when(peer > me)
                        def _():
                            pl.semaphore_wait(ready.at[peer], 1)

                    @pl.when(peer != me)
                    def _():
                        pltpu.make_async_remote_copy(
                            src_ref=x_ref.at[peer * images + image], dst_ref=hid.at[image, my_rows, :],
                            send_sem=in_send, recv_sem=in_recv.at[image],
                            device_id={'sp': peer}, device_id_type=MESH).start()
        pltpu.make_async_copy(x_ref.at[me * images + image], hid.at[image, my_rows, :], in_recv.at[image]).start()

    for copy in params:
        copy.start()
    for copy in weight_copies(0):
        copy.start()

    barrier = pltpu.get_barrier_semaphore()

    @pl.loop(me + 1, peers)
    def _(peer):
        pl.semaphore_signal(barrier, inc=1, device_id={'sp': peer}, device_id_type=MESH)

    @pl.when(me > 0)
    def _():
        pl.semaphore_wait(barrier, me)

    @pl.loop(0, me)
    def _(peer):
        pl.semaphore_signal(ready.at[me], inc=1, device_id={'sp': peer}, device_id_type=MESH)

    send_in(0, True)
    for layer in range(1, layers):
        for copy in weight_copies(layer):
            copy.start()
    for copy in params:
        copy.wait()

    def body(step_idx, carry):
        image = step_idx // layers
        layer = lax.rem(step_idx, layers)
        state = hid.at[image]

        @pl.when(image == 0)
        def _():
            for copy in weight_copies(layer)[:2]:
                copy.wait()

        @pl.when(layer == 0)
        def _():
            pltpu.make_async_copy(state, state, in_recv.at[image]).wait()

        row = pl.ds(layer, 1)
        norm_rows(state, normed, g1[row, :], s1[row, :], 32)

        for slot, dst in ((0, q_t), (2, v_t)):
            bias = bqkv[layer, slot].T
            for start in range(0, width, 512):
                part = lax.dot_general(wqkv[layer, pl.ds(slot * width + start, 512), :], normed[...], NT, preferred_element_type=F32)
                for off in range(0, 512, head_dim):
                    head = (start + off) // head_dim
                    dst[pl.ds(start + off, head_dim), :] = (part[off:off + head_dim] + bias[:, head:head + 1]).astype(BF)
        for start in range(0, width, 512):
            part = lax.dot_general(normed[...], wqkv[layer, pl.ds(width + start, 512), :], NT, preferred_element_type=F32)
            bias = jnp.concatenate([bqkv[layer, 1, pl.ds((start + off) // head_dim, 1), :] for off in range(0, 512, head_dim)], axis=-1)
            keys[:, pl.ds(start, 512)] = (part + bias).astype(BF)

        scale = head_dim ** -0.5 / math.log(2.0)
        zeros = jnp.zeros((head_dim, tokens), BF)

        def score(head):
            pair = head // 2 * 2
            q_head = q_t[pl.ds(head * head_dim, head_dim), :]
            rhs = jnp.concatenate([q_head, zeros] if head == pair else [zeros, q_head], axis=0)
            part = jnp.dot(keys[:, pl.ds(pair * head_dim, 2 * head_dim)], rhs, preferred_element_type=F32)
            scores[head % 4] = part
            peaks[head % 4] = jnp.max(part, axis=0, keepdims=True)

        def soften(head):
            prob = jnp.exp2((scores[head % 4] - peaks[head % 4]) * scale)
            totals[head % 4] = jnp.sum(prob, axis=0, keepdims=True)
            probs[head % 4] = prob.astype(BF)

        def mix(head):
            part = jnp.dot(v_t[pl.ds(head * head_dim, head_dim), :], probs[head % 4], preferred_element_type=F32)
            mixed_t[pl.ds(head * head_dim, head_dim), :] = part * (1.0 / totals[head % 4])

        for step in range(0, heads + 4, 2):
            for head in (step, step + 1):
                if head < heads:
                    score(head)
            for head in (step - 2, step - 1):
                if 0 <= head < heads:
                    soften(head)
            for head in (step - 4, step - 3):
                if 0 <= head < heads:
                    mix(head)
            if step >= 4:
                cols = pl.ds((step - 4) * head_dim, 2 * head_dim)
                mixed[:, cols] = mixed_t[cols, :].T.astype(BF)

        for start in range(0, width, 512):
            cols = pl.ds(start, 512)
            part = jnp.dot(mixed[...], wout[layer, :, cols], preferred_element_type=F32) + bout[row, cols]
            state[:, cols] = (state[:, cols].astype(F32) + part).astype(BF)

        @pl.when(image == 0)
        def _():
            for copy in weight_copies(layer)[2:]:
                copy.wait()

        @pl.when(step_idx == 0)
        def _():
            for other in range(1, images):
                send_in(other, False)

        norm_rows(state, normed, g2[row, :], s2[row, :], 32)
        for start in range(0, mlp_dim, 512):
            cols = pl.ds(start, 512)
            part = jnp.dot(normed[...], wup[layer, :, cols], preferred_element_type=F32) + bup[row, cols]
            active[:, cols] = gelu(part).astype(BF)
        for start in range(0, width, 512):
            cols = pl.ds(start, 512)
            part = jnp.dot(active[...], wdown[layer, :, cols], preferred_element_type=F32) + bdown[row, cols]
            state[:, cols] = (state[:, cols].astype(F32) + part).astype(BF)

        @pl.when(layer == layers - 1)
        def _():
            slot = me * images + image

            for hop in sorted(hops(peers, 0) + hops(peers, 1), key=lambda hop: (-min(hop, peers // 2 - hop), hop)):
                for core in range(2):
                    peer = 2 * lax.rem(me // 2 + hop, peers // 2) + core
                    rows = pl.ds(pl.multiple_of(peer * block, block), block)

                    @pl.when(peer != me)
                    def _():
                        pltpu.make_async_remote_copy(
                            src_ref=hid.at[image, rows, :], dst_ref=out_ref.at[slot],
                            send_sem=out_send, recv_sem=out_recv,
                            device_id={'sp': peer}, device_id_type=MESH).start()

            out_ref[slot] = hid[image, my_rows, :]

        return carry

    lax.fori_loop(0, images * layers, body, 0)

    sent = x_ref.at[pl.ds(0, (peers - 1) * images)]
    pltpu.make_async_copy(sent, sent, in_send).wait()
    pltpu.make_async_copy(sent, sent, out_send).wait()
    pltpu.make_async_copy(sent, sent, out_recv).wait()


def solution(mesh):
    token_spec = P('dp', 'sp', None)
    peers = mesh.shape['sp']

    def device_step(image_tokens, ln1_gain, ln1_shift, w_qkv, b_qkv, w_out, b_out, ln2_gain, ln2_shift, w_up, b_up, w_down, b_down):
        total_images, block, width = image_tokens.shape
        layers, _, _, heads, head_dim = w_qkv.shape
        mlp_dim = w_up.shape[-1]
        images = total_images // peers
        tokens = block * peers
        inner = heads * head_dim
        w_qkv_t = jnp.transpose(w_qkv, (0, 2, 3, 4, 1)).reshape(layers, 3 * inner, width)
        w_out_m = w_out.reshape(layers, inner, width)
        args = (image_tokens, ln1_gain, ln1_shift, w_qkv_t, b_qkv, w_out_m, b_out, ln2_gain, ln2_shift, w_up, b_up, w_down, b_down)
        small = lambda a: pltpu.VMEM(a.shape, a.dtype)
        return pl.pallas_call(
            functools.partial(kernel, peers),
            out_shape=pltpu.VMEM(image_tokens.shape, image_tokens.dtype),
            in_specs=[pl.BlockSpec(memory_space=pl.ANY)] * len(args),
            out_specs=pl.BlockSpec(memory_space=pltpu.VMEM),
            scratch_shapes=[
                pltpu.VMEM((images, tokens, width), BF),
                small(w_qkv_t), small(w_out_m), small(w_up), small(w_down),
                small(ln1_gain), small(ln1_shift), small(b_qkv), small(b_out), small(ln2_gain), small(ln2_shift), small(b_up), small(b_down),
                pltpu.VMEM((tokens, width), BF),
                pltpu.VMEM((inner, tokens), BF),
                pltpu.VMEM((inner, tokens), BF),
                pltpu.VMEM((tokens, inner), BF),
                pltpu.VMEM((tokens, inner), BF),
                pltpu.VMEM((tokens, mlp_dim), BF),
                pltpu.VMEM((4, tokens, tokens), F32),
                pltpu.VMEM((4, tokens, tokens), BF),
                pltpu.VMEM((4, 1, tokens), F32),
                pltpu.VMEM((4, 1, tokens), F32),
                pltpu.VMEM((inner, tokens), F32),
                pltpu.SemaphoreType.REGULAR((peers,)),
                pltpu.SemaphoreType.DMA((layers, 4)),
                pltpu.SemaphoreType.DMA((8,)),
                pltpu.SemaphoreType.DMA,
                pltpu.SemaphoreType.DMA((images,)),
                pltpu.SemaphoreType.DMA,
                pltpu.SemaphoreType.DMA,
            ],
            compiler_params=pltpu.CompilerParams(collective_id=0, has_side_effects=True, vmem_limit_bytes=65_500_000),
        )(*args)

    return jax.shard_map(device_step, mesh=mesh, in_specs=(token_spec,) + (P(),) * 12, out_specs=token_spec, check_vma=False)
```

```python
import functools
import math

import jax
import jax.numpy as jnp
from jax import lax
from jax.experimental import pallas as pl
from jax.experimental.pallas import tpu as pltpu
from jax.sharding import PartitionSpec as P

LN_EPS = 1e-6
MESH = pl.DeviceIdType.MESH
BF = jnp.bfloat16
F32 = jnp.float32
NT = (((1,), (1,)), ((), ()))


def norm_rows(src, dst, gain, shift, rows):
    total = src.shape[0]
    width = src.shape[1]
    for start in range(0, total, rows):
        values = src[pl.ds(start, rows), :].astype(F32)
        mean_val = jnp.sum(values, axis=-1, keepdims=True) * (1.0 / width)
        centred = values - mean_val
        var_val = jnp.sum(centred * centred, axis=-1, keepdims=True) * (1.0 / width)
        dst[pl.ds(start, rows), :] = (centred * lax.rsqrt(var_val + LN_EPS) * gain + shift).astype(BF)


def gelu(x):
    c0 = math.sqrt(2.0 / math.pi)
    c1 = c0 * 0.044715
    return 0.5 * x * (1.0 + jnp.tanh(x * (c0 + c1 * (x * x))))


def hops(peers, parity):
    chips = peers // 2
    return sorted(range(parity, chips, 2), key=lambda hop: (-min(hop, chips - hop), hop))


def kernel(peers, x_ref, g1_hbm, s1_hbm, wqkv_hbm, bqkv_hbm, wout_hbm, bout_hbm, g2_hbm, s2_hbm, wup_hbm, bup_hbm, wdown_hbm, bdown_hbm,
           out_ref,
           hid, wqkv, wout, wup, wdown, g1, s1, bqkv, bout, g2, s2, bup, bdown,
           normed, q_t, v_t, keys, mixed, active, scores, probs, peaks, totals, mixed_t,
           ready, w_sem, p_sem, in_send, in_recv, out_send, out_recv):
    images = hid.shape[0]
    block = x_ref.shape[1]
    layers, heads, head_dim = bqkv.shape[0], bqkv.shape[2], bqkv.shape[3]
    tokens, width = hid.shape[1], hid.shape[2]
    mlp_dim = wup.shape[2]
    me = lax.axis_index('sp')

    params = [pltpu.make_async_copy(src, dst, p_sem.at[i]) for i, (src, dst) in enumerate((
        (g1_hbm, g1), (s1_hbm, s1), (bqkv_hbm, bqkv), (bout_hbm, bout), (g2_hbm, g2), (s2_hbm, s2), (bup_hbm, bup), (bdown_hbm, bdown)))]

    def weight_copies(layer):
        return [pltpu.make_async_copy(src.at[layer], dst.at[layer], w_sem.at[layer, i]) for i, (src, dst) in enumerate((
            (wqkv_hbm, wqkv), (wout_hbm, wout), (wup_hbm, wup), (wdown_hbm, wdown)))]

    my_rows = pl.ds(pl.multiple_of(me * block, block), block)

    def send_in(image, ask):
        for core in range(2):
            for parity in range(2):
                odd = lax.rem(me // 2 + parity, 2)
                for even_hop, odd_hop in zip(hops(peers, 0), hops(peers, 1)):
                    peer = 2 * lax.rem(me // 2 + even_hop + odd * (odd_hop - even_hop), peers // 2) + core

                    if ask:
                        @pl.when(peer > me)
                        def _():
                            pl.semaphore_wait(ready.at[peer], 1)

                    @pl.when(peer != me)
                    def _():
                        pltpu.make_async_remote_copy(
                            src_ref=x_ref.at[peer * images + image], dst_ref=hid.at[image, my_rows, :],
                            send_sem=in_send, recv_sem=in_recv.at[image],
                            device_id={'sp': peer}, device_id_type=MESH).start()
        pltpu.make_async_copy(x_ref.at[me * images + image], hid.at[image, my_rows, :], in_recv.at[image]).start()

    for copy in params:
        copy.start()
    for copy in weight_copies(0):
        copy.start()

    barrier = pltpu.get_barrier_semaphore()

    @pl.loop(me + 1, peers)
    def _(peer):
        pl.semaphore_signal(barrier, inc=1, device_id={'sp': peer}, device_id_type=MESH)

    @pl.when(me > 0)
    def _():
        pl.semaphore_wait(barrier, me)

    @pl.loop(0, me)
    def _(peer):
        pl.semaphore_signal(ready.at[me], inc=1, device_id={'sp': peer}, device_id_type=MESH)

    send_in(0, True)
    for layer in range(1, layers):
        for copy in weight_copies(layer):
            copy.start()
    for copy in params:
        copy.wait()

    def body(step_idx, carry):
        image = step_idx // layers
        layer = lax.rem(step_idx, layers)
        state = hid.at[image]

        @pl.when(image == 0)
        def _():
            for copy in weight_copies(layer)[:2]:
                copy.wait()

        @pl.when(layer == 0)
        def _():
            pltpu.make_async_copy(state, state, in_recv.at[image]).wait()

        row = pl.ds(layer, 1)
        norm_rows(state, normed, g1[row, :], s1[row, :], 32)

        group = 256
        group_heads = group // head_dim
        bias_q, bias_v = bqkv[layer, 0].T, bqkv[layer, 2].T

        def make_rows(slot, bias, dst, index):
            start = index * group
            part = lax.dot_general(wqkv[layer, pl.ds(slot * width + start, group), :], normed[...], NT, preferred_element_type=F32)
            for off in range(0, group, head_dim):
                head = (start + off) // head_dim
                dst[pl.ds(start + off, head_dim), :] = (part[off:off + head_dim] + bias[:, head:head + 1]).astype(BF)

        def make_keys(index):
            start = index * group
            part = lax.dot_general(normed[...], wqkv[layer, pl.ds(width + start, group), :], NT, preferred_element_type=F32)
            bias = jnp.concatenate([bqkv[layer, 1, pl.ds((start + off) // head_dim, 1), :] for off in range(0, group, head_dim)], axis=-1)
            keys[:, pl.ds(start, group)] = (part + bias).astype(BF)

        scale = head_dim ** -0.5 / math.log(2.0)
        zeros = jnp.zeros((head_dim, tokens), BF)

        def score(head):
            pair = head // 2 * 2
            q_head = q_t[pl.ds(head * head_dim, head_dim), :]
            rhs = jnp.concatenate([q_head, zeros] if head == pair else [zeros, q_head], axis=0)
            part = jnp.dot(keys[:, pl.ds(pair * head_dim, 2 * head_dim)], rhs, preferred_element_type=F32)
            scores[head % 4] = part
            peaks[head % 4] = jnp.max(part, axis=0, keepdims=True)

        def soften(head):
            prob = jnp.exp2((scores[head % 4] - peaks[head % 4]) * scale)
            totals[head % 4] = jnp.sum(prob, axis=0, keepdims=True)
            probs[head % 4] = prob.astype(BF)

        def mix(head):
            part = jnp.dot(v_t[pl.ds(head * head_dim, head_dim), :], probs[head % 4], preferred_element_type=F32)
            mixed_t[pl.ds(head * head_dim, head_dim), :] = part * (1.0 / totals[head % 4])

        make_rows(0, bias_q, q_t, 0)
        make_keys(0)
        make_rows(2, bias_v, v_t, 0)
        for step in range(0, heads + 4, 2):
            for head in (step, step + 1):
                if head < heads:
                    score(head)
            ahead = step // group_heads + 1
            if ahead * group < width:
                if step % group_heads == 0:
                    make_rows(0, bias_q, q_t, ahead)
                    make_keys(ahead)
                else:
                    make_rows(2, bias_v, v_t, ahead)
            for head in (step - 2, step - 1):
                if 0 <= head < heads:
                    soften(head)
            for head in (step - 4, step - 3):
                if 0 <= head < heads:
                    mix(head)
            if step >= 4:
                cols = pl.ds((step - 4) * head_dim, 2 * head_dim)
                mixed[:, cols] = mixed_t[cols, :].T.astype(BF)

        for start in range(0, width, 512):
            cols = pl.ds(start, 512)
            part = jnp.dot(mixed[...], wout[layer, :, cols], preferred_element_type=F32) + bout[row, cols]
            state[:, cols] = (state[:, cols].astype(F32) + part).astype(BF)

        @pl.when(image == 0)
        def _():
            for copy in weight_copies(layer)[2:]:
                copy.wait()

        @pl.when(step_idx == 0)
        def _():
            for other in range(1, images):
                send_in(other, False)

        norm_rows(state, normed, g2[row, :], s2[row, :], 32)
        for start in range(0, mlp_dim, 512):
            cols = pl.ds(start, 512)
            part = jnp.dot(normed[...], wup[layer, :, cols], preferred_element_type=F32) + bup[row, cols]
            active[:, cols] = gelu(part).astype(BF)
        for start in range(0, width, 512):
            cols = pl.ds(start, 512)
            part = jnp.dot(active[...], wdown[layer, :, cols], preferred_element_type=F32) + bdown[row, cols]
            state[:, cols] = (state[:, cols].astype(F32) + part).astype(BF)

        @pl.when(layer == layers - 1)
        def _():
            slot = me * images + image

            def give(peer):
                rows = pl.ds(pl.multiple_of(peer * block, block), block)
                pltpu.make_async_remote_copy(
                    src_ref=hid.at[image, rows, :], dst_ref=out_ref.at[slot],
                    send_sem=out_send, recv_sem=out_recv,
                    device_id={'sp': peer}, device_id_type=MESH).start()

            for peer in (1, 0):
                @pl.when(peer != me)
                def _():
                    give(peer)

            for hop in sorted(range(peers // 2), key=lambda hop: (-min(hop, peers // 2 - hop), hop)):
                for core in range(2):
                    peer = 2 * lax.rem(me // 2 + hop, peers // 2) + core

                    @pl.when(jnp.logical_and(peer != me, peer > 1))
                    def _():
                        give(peer)

            out_ref[slot] = hid[image, my_rows, :]

        return carry

    lax.fori_loop(0, images * layers, body, 0)

    sent = x_ref.at[pl.ds(0, (peers - 1) * images)]
    pltpu.make_async_copy(sent, sent, in_send).wait()
    pltpu.make_async_copy(sent, sent, out_send).wait()
    pltpu.make_async_copy(sent, sent, out_recv).wait()


def solution(mesh):
    token_spec = P('dp', 'sp', None)
    peers = mesh.shape['sp']

    def device_step(image_tokens, ln1_gain, ln1_shift, w_qkv, b_qkv, w_out, b_out, ln2_gain, ln2_shift, w_up, b_up, w_down, b_down):
        total_images, block, width = image_tokens.shape
        layers, _, _, heads, head_dim = w_qkv.shape
        mlp_dim = w_up.shape[-1]
        images = total_images // peers
        tokens = block * peers
        inner = heads * head_dim
        w_qkv_t = jnp.transpose(w_qkv, (0, 2, 3, 4, 1)).reshape(layers, 3 * inner, width)
        w_out_m = w_out.reshape(layers, inner, width)
        args = (image_tokens, ln1_gain, ln1_shift, w_qkv_t, b_qkv, w_out_m, b_out, ln2_gain, ln2_shift, w_up, b_up, w_down, b_down)
        small = lambda a: pltpu.VMEM(a.shape, a.dtype)
        return pl.pallas_call(
            functools.partial(kernel, peers),
            out_shape=pltpu.VMEM(image_tokens.shape, image_tokens.dtype),
            in_specs=[pl.BlockSpec(memory_space=pl.ANY)] * len(args),
            out_specs=pl.BlockSpec(memory_space=pltpu.VMEM),
            scratch_shapes=[
                pltpu.VMEM((images, tokens, width), BF),
                small(w_qkv_t), small(w_out_m), small(w_up), small(w_down),
                small(ln1_gain), small(ln1_shift), small(b_qkv), small(b_out), small(ln2_gain), small(ln2_shift), small(b_up), small(b_down),
                pltpu.VMEM((tokens, width), BF),
                pltpu.VMEM((inner, tokens), BF),
                pltpu.VMEM((inner, tokens), BF),
                pltpu.VMEM((tokens, inner), BF),
                pltpu.VMEM((tokens, inner), BF),
                pltpu.VMEM((tokens, mlp_dim), BF),
                pltpu.VMEM((4, tokens, tokens), F32),
                pltpu.VMEM((4, tokens, tokens), BF),
                pltpu.VMEM((4, 1, tokens), F32),
                pltpu.VMEM((4, 1, tokens), F32),
                pltpu.VMEM((inner, tokens), F32),
                pltpu.SemaphoreType.REGULAR((peers,)),
                pltpu.SemaphoreType.DMA((layers, 4)),
                pltpu.SemaphoreType.DMA((8,)),
                pltpu.SemaphoreType.DMA,
                pltpu.SemaphoreType.DMA((images,)),
                pltpu.SemaphoreType.DMA,
                pltpu.SemaphoreType.DMA,
            ],
            compiler_params=pltpu.CompilerParams(collective_id=0, has_side_effects=True, vmem_limit_bytes=65_500_000),
        )(*args)

    return jax.shard_map(device_step, mesh=mesh, in_specs=(token_spec,) + (P(),) * 12, out_specs=token_spec, check_vma=False)
```

```python
import functools
import math

import jax
import jax.numpy as jnp
from jax import lax
from jax.experimental import pallas as pl
from jax.experimental.pallas import tpu as pltpu
from jax.sharding import PartitionSpec as P

LN_EPS = 1e-6
MESH = pl.DeviceIdType.MESH
BF = jnp.bfloat16
F32 = jnp.float32
NT = (((1,), (1,)), ((), ()))


def norm_rows(src, dst, gain, shift, rows):
    total = src.shape[0]
    width = src.shape[1]
    for start in range(0, total, rows):
        values = src[pl.ds(start, rows), :].astype(F32)
        mean_val = jnp.sum(values, axis=-1, keepdims=True) * (1.0 / width)
        centred = values - mean_val
        var_val = jnp.sum(centred * centred, axis=-1, keepdims=True) * (1.0 / width)
        dst[pl.ds(start, rows), :] = (centred * lax.rsqrt(var_val + LN_EPS) * gain + shift).astype(BF)


def gelu(x):
    c0 = math.sqrt(2.0 / math.pi)
    c1 = c0 * 0.044715
    return 0.5 * x * (1.0 + jnp.tanh(x * (c0 + c1 * (x * x))))


def hops(peers, parity):
    chips = peers // 2
    return sorted(range(parity, chips, 2), key=lambda hop: (-min(hop, chips - hop), hop))


def when(cond):
    if isinstance(cond, bool):
        return (lambda run: run()) if cond else (lambda run: None)
    return pl.when(cond)


def kernel(peers, x_ref, g1_hbm, s1_hbm, wqkv_hbm, bqkv_hbm, wout_hbm, bout_hbm, g2_hbm, s2_hbm, wup_hbm, bup_hbm, wdown_hbm, bdown_hbm,
           out_ref,
           hid, wqkv, wout, wup, wdown, g1, s1, bqkv, bout, g2, s2, bup, bdown,
           normed, q_t, v_t, keys, mixed, active, scores, probs, peaks, totals, mixed_t,
           ready, w_sem, p_sem, in_send, in_recv, out_send, out_recv):
    images = hid.shape[0]
    block = x_ref.shape[1]
    layers, heads, head_dim = bqkv.shape[0], bqkv.shape[2], bqkv.shape[3]
    tokens, width = hid.shape[1], hid.shape[2]
    mlp_dim = wup.shape[2]
    me = lax.axis_index('sp')

    params = [pltpu.make_async_copy(src, dst, p_sem.at[i]) for i, (src, dst) in enumerate((
        (g1_hbm, g1), (s1_hbm, s1), (bqkv_hbm, bqkv), (bout_hbm, bout), (g2_hbm, g2), (s2_hbm, s2), (bup_hbm, bup), (bdown_hbm, bdown)))]

    def weight_copies(layer):
        return [pltpu.make_async_copy(src.at[layer], dst.at[layer], w_sem.at[layer, i]) for i, (src, dst) in enumerate((
            (wqkv_hbm, wqkv), (wout_hbm, wout), (wup_hbm, wup), (wdown_hbm, wdown)))]

    my_rows = pl.ds(pl.multiple_of(me * block, block), block)

    def send_in(image, ask):
        for core in range(2):
            for parity in range(2):
                odd = lax.rem(me // 2 + parity, 2)
                for even_hop, odd_hop in zip(hops(peers, 0), hops(peers, 1)):
                    peer = 2 * lax.rem(me // 2 + even_hop + odd * (odd_hop - even_hop), peers // 2) + core

                    if ask:
                        @pl.when(peer > me)
                        def _():
                            pl.semaphore_wait(ready.at[peer], 1)

                    @pl.when(peer != me)
                    def _():
                        pltpu.make_async_remote_copy(
                            src_ref=x_ref.at[peer * images + image], dst_ref=hid.at[image, my_rows, :],
                            send_sem=in_send, recv_sem=in_recv.at[image],
                            device_id={'sp': peer}, device_id_type=MESH).start()
        pltpu.make_async_copy(x_ref.at[me * images + image], hid.at[image, my_rows, :], in_recv.at[image]).start()

    for copy in params:
        copy.start()
    for copy in weight_copies(0):
        copy.start()

    barrier = pltpu.get_barrier_semaphore()

    @pl.loop(me + 1, peers)
    def _(peer):
        pl.semaphore_signal(barrier, inc=1, device_id={'sp': peer}, device_id_type=MESH)

    @pl.when(me > 0)
    def _():
        pl.semaphore_wait(barrier, me)

    @pl.loop(0, me)
    def _(peer):
        pl.semaphore_signal(ready.at[me], inc=1, device_id={'sp': peer}, device_id_type=MESH)

    send_in(0, True)
    for layer in range(1, layers):
        for copy in weight_copies(layer):
            copy.start()
    for copy in params:
        copy.wait()

    def body(step_idx):
        last = isinstance(step_idx, int)
        image = step_idx // layers
        layer = step_idx % layers if last else lax.rem(step_idx, layers)
        state = hid.at[image]

        @when(image == 0)
        def _():
            for copy in weight_copies(layer)[:2]:
                copy.wait()

        @when(layer == 0)
        def _():
            pltpu.make_async_copy(state, state, in_recv.at[image]).wait()

        row = pl.ds(layer, 1)
        norm_rows(state, normed, g1[row, :], s1[row, :], 32)

        group = 256
        group_heads = group // head_dim
        bias_q, bias_v = bqkv[layer, 0].T, bqkv[layer, 2].T

        def make_rows(slot, bias, dst, index):
            start = index * group
            part = lax.dot_general(wqkv[layer, pl.ds(slot * width + start, group), :], normed[...], NT, preferred_element_type=F32)
            for off in range(0, group, head_dim):
                head = (start + off) // head_dim
                dst[pl.ds(start + off, head_dim), :] = (part[off:off + head_dim] + bias[:, head:head + 1]).astype(BF)

        def make_keys(index):
            start = index * group
            part = lax.dot_general(normed[...], wqkv[layer, pl.ds(width + start, group), :], NT, preferred_element_type=F32)
            bias = jnp.concatenate([bqkv[layer, 1, pl.ds((start + off) // head_dim, 1), :] for off in range(0, group, head_dim)], axis=-1)
            keys[:, pl.ds(start, group)] = (part + bias).astype(BF)

        scale = head_dim ** -0.5 / math.log(2.0)
        zeros = jnp.zeros((head_dim, tokens), BF)

        def score(head):
            pair = head // 2 * 2
            q_head = q_t[pl.ds(head * head_dim, head_dim), :]
            rhs = jnp.concatenate([q_head, zeros] if head == pair else [zeros, q_head], axis=0)
            part = jnp.dot(keys[:, pl.ds(pair * head_dim, 2 * head_dim)], rhs, preferred_element_type=F32)
            scores[head % 4] = part
            peaks[head % 4] = jnp.max(part, axis=0, keepdims=True)

        def soften(head):
            prob = jnp.exp2((scores[head % 4] - peaks[head % 4]) * scale)
            totals[head % 4] = jnp.sum(prob, axis=0, keepdims=True)
            probs[head % 4] = prob.astype(BF)

        def mix(head):
            part = jnp.dot(v_t[pl.ds(head * head_dim, head_dim), :], probs[head % 4], preferred_element_type=F32)
            mixed_t[pl.ds(head * head_dim, head_dim), :] = part * (1.0 / totals[head % 4])

        make_rows(0, bias_q, q_t, 0)
        make_keys(0)
        make_rows(2, bias_v, v_t, 0)
        for step in range(0, heads + 4, 2):
            for head in (step, step + 1):
                if head < heads:
                    score(head)
            ahead = step // group_heads + 1
            if ahead * group < width:
                if step % group_heads == 0:
                    make_rows(0, bias_q, q_t, ahead)
                    make_keys(ahead)
                else:
                    make_rows(2, bias_v, v_t, ahead)
            for head in (step - 2, step - 1):
                if 0 <= head < heads:
                    soften(head)
            for head in (step - 4, step - 3):
                if 0 <= head < heads:
                    mix(head)
            if step >= 4:
                cols = pl.ds((step - 4) * head_dim, 2 * head_dim)
                mixed[:, cols] = mixed_t[cols, :].T.astype(BF)

        for start in range(0, width, 512):
            cols = pl.ds(start, 512)
            part = jnp.dot(mixed[...], wout[layer, :, cols], preferred_element_type=F32) + bout[row, cols]
            state[:, cols] = (state[:, cols].astype(F32) + part).astype(BF)

        @when(image == 0)
        def _():
            for copy in weight_copies(layer)[2:]:
                copy.wait()

        @when(step_idx == 0)
        def _():
            for other in range(1, images):
                send_in(other, False)

        slot = me * images + image

        def give(peer):
            rows = pl.ds(pl.multiple_of(peer * block, block), block)
            pltpu.make_async_remote_copy(
                src_ref=hid.at[image, rows, :], dst_ref=out_ref.at[slot],
                send_sem=out_send, recv_sem=out_recv,
                device_id={'sp': peer}, device_id_type=MESH).start()

        def leave():
            for peer in (1, 0):
                @pl.when(peer != me)
                def _():
                    give(peer)

            for hop in sorted(range(peers // 2), key=lambda hop: (-min(hop, peers // 2 - hop), hop)):
                for core in range(2):
                    peer = 2 * lax.rem(me // 2 + hop, peers // 2) + core

                    @pl.when(jnp.logical_and(peer != me, peer > 1))
                    def _():
                        give(peer)

            out_ref[slot] = hid[image, my_rows, :]

        def leave_part(part):
            count = peers // 4
            for turn in range(count):
                index = lax.rem(me // 2 + turn, count)
                chip = index // (count // 2) * count + part * (count // 2) + lax.rem(index, count // 2)
                for core in range(2):
                    peer = 2 * chip + core

                    @pl.when(peer != me)
                    def _():
                        give(peer)

            @pl.when(lax.rem(me // count, 2) == part)
            def _():
                out_ref[slot] = hid[image, my_rows, :]

        if last:
            quarter = tokens // 4

            def norm_part(part):
                for index in range(2):
                    norm_rows(state.at[pl.ds((2 * index + part) * quarter, quarter), :],
                              normed.at[pl.ds((2 * part + index) * quarter, quarter), :], g2[row, :], s2[row, :], 32)

            def widen_part(part):
                rows = pl.ds(2 * part * quarter, 2 * quarter)
                for start in range(0, mlp_dim, 512):
                    cols = pl.ds(start, 512)
                    part_up = jnp.dot(normed[rows, :], wup[layer, :, cols], preferred_element_type=F32) + bup[row, cols]
                    active[rows, cols] = gelu(part_up).astype(BF)

            def narrow_part(part):
                for start in range(0, width, 512):
                    cols = pl.ds(start, 512)
                    part_down = jnp.dot(active[pl.ds(2 * part * quarter, 2 * quarter), :], wdown[layer, :, cols], preferred_element_type=F32) + bdown[row, cols]
                    for index in range(2):
                        rows = pl.ds((2 * index + part) * quarter, quarter)
                        state[rows, cols] = (state[rows, cols].astype(F32) + part_down[index * quarter:(index + 1) * quarter]).astype(BF)

            norm_part(0)
            widen_part(0)
            norm_part(1)
            narrow_part(0)
            leave_part(0)
            widen_part(1)
            narrow_part(1)
            leave_part(1)
        else:
            norm_rows(state, normed, g2[row, :], s2[row, :], 32)
            for start in range(0, mlp_dim, 512):
                cols = pl.ds(start, 512)
                part = jnp.dot(normed[...], wup[layer, :, cols], preferred_element_type=F32) + bup[row, cols]
                active[:, cols] = gelu(part).astype(BF)
            for start in range(0, width, 512):
                cols = pl.ds(start, 512)
                part = jnp.dot(active[...], wdown[layer, :, cols], preferred_element_type=F32) + bdown[row, cols]
                state[:, cols] = (state[:, cols].astype(F32) + part).astype(BF)

            pl.when(layer == layers - 1)(leave)

    @pl.loop(0, images * layers - 1)
    def _(step_idx):
        body(step_idx)

    body(images * layers - 1)

    sent = x_ref.at[pl.ds(0, (peers - 1) * images)]
    pltpu.make_async_copy(sent, sent, in_send).wait()
    pltpu.make_async_copy(sent, sent, out_send).wait()
    pltpu.make_async_copy(sent, sent, out_recv).wait()


def solution(mesh):
    token_spec = P('dp', 'sp', None)
    peers = mesh.shape['sp']

    def device_step(image_tokens, ln1_gain, ln1_shift, w_qkv, b_qkv, w_out, b_out, ln2_gain, ln2_shift, w_up, b_up, w_down, b_down):
        total_images, block, width = image_tokens.shape
        layers, _, _, heads, head_dim = w_qkv.shape
        mlp_dim = w_up.shape[-1]
        images = total_images // peers
        tokens = block * peers
        inner = heads * head_dim
        w_qkv_t = jnp.transpose(w_qkv, (0, 2, 3, 4, 1)).reshape(layers, 3 * inner, width)
        w_out_m = w_out.reshape(layers, inner, width)
        args = (image_tokens, ln1_gain, ln1_shift, w_qkv_t, b_qkv, w_out_m, b_out, ln2_gain, ln2_shift, w_up, b_up, w_down, b_down)
        small = lambda a: pltpu.VMEM(a.shape, a.dtype)
        return pl.pallas_call(
            functools.partial(kernel, peers),
            out_shape=pltpu.VMEM(image_tokens.shape, image_tokens.dtype),
            in_specs=[pl.BlockSpec(memory_space=pl.ANY)] * len(args),
            out_specs=pl.BlockSpec(memory_space=pltpu.VMEM),
            scratch_shapes=[
                pltpu.VMEM((images, tokens, width), BF),
                small(w_qkv_t), small(w_out_m), small(w_up), small(w_down),
                small(ln1_gain), small(ln1_shift), small(b_qkv), small(b_out), small(ln2_gain), small(ln2_shift), small(b_up), small(b_down),
                pltpu.VMEM((tokens, width), BF),
                pltpu.VMEM((inner, tokens), BF),
                pltpu.VMEM((inner, tokens), BF),
                pltpu.VMEM((tokens, inner), BF),
                pltpu.VMEM((tokens, inner), BF),
                pltpu.VMEM((tokens, mlp_dim), BF),
                pltpu.VMEM((4, tokens, tokens), F32),
                pltpu.VMEM((4, tokens, tokens), BF),
                pltpu.VMEM((4, 1, tokens), F32),
                pltpu.VMEM((4, 1, tokens), F32),
                pltpu.VMEM((inner, tokens), F32),
                pltpu.SemaphoreType.REGULAR((peers,)),
                pltpu.SemaphoreType.DMA((layers, 4)),
                pltpu.SemaphoreType.DMA((8,)),
                pltpu.SemaphoreType.DMA,
                pltpu.SemaphoreType.DMA((images,)),
                pltpu.SemaphoreType.DMA,
                pltpu.SemaphoreType.DMA,
            ],
            compiler_params=pltpu.CompilerParams(collective_id=0, has_side_effects=True, vmem_limit_bytes=65_500_000),
        )(*args)

    return jax.shard_map(device_step, mesh=mesh, in_specs=(token_spec,) + (P(),) * 12, out_specs=token_spec, check_vma=False)
```

```python
import functools
import math

import jax
import jax.numpy as jnp
from jax import lax
from jax.experimental import pallas as pl
from jax.experimental.pallas import tpu as pltpu
from jax.sharding import PartitionSpec as P

LN_EPS = 1e-6
MESH = pl.DeviceIdType.MESH
BF = jnp.bfloat16
F32 = jnp.float32
NT = (((1,), (1,)), ((), ()))


def norm_rows(src, dst, gain, shift, rows):
    total = src.shape[0]
    width = src.shape[1]
    for start in range(0, total, rows):
        values = src[pl.ds(start, rows), :].astype(F32)
        mean_val = jnp.sum(values, axis=-1, keepdims=True) * (1.0 / width)
        centred = values - mean_val
        var_val = jnp.sum(centred * centred, axis=-1, keepdims=True) * (1.0 / width)
        dst[pl.ds(start, rows), :] = (centred * lax.rsqrt(var_val + LN_EPS) * gain + shift).astype(BF)


def gelu(x):
    c0 = math.sqrt(2.0 / math.pi)
    c1 = c0 * 0.044715
    return 0.5 * x * (1.0 + jnp.tanh(x * (c0 + c1 * (x * x))))


def hops(peers, parity):
    chips = peers // 2
    return sorted(range(parity, chips, 2), key=lambda hop: (-min(hop, chips - hop), hop))


def when(cond):
    if isinstance(cond, bool):
        return (lambda run: run()) if cond else (lambda run: None)
    return pl.when(cond)


def kernel(peers, x_ref, g1_hbm, s1_hbm, wqkv_hbm, bqkv_hbm, wout_hbm, bout_hbm, g2_hbm, s2_hbm, wup_hbm, bup_hbm, wdown_hbm, bdown_hbm,
           out_ref,
           hid, wqkv, wout, wup, wdown, g1, s1, bqkv, bout, g2, s2, bup, bdown,
           normed, q_t, v_t, keys, mixed, active, scores, probs, peaks, totals, mixed_t,
           ready, w_sem, p_sem, in_send, in_recv, out_send, out_recv):
    images = hid.shape[0]
    block = x_ref.shape[1]
    layers, heads, head_dim = bqkv.shape[0], bqkv.shape[2], bqkv.shape[3]
    tokens, width = hid.shape[1], hid.shape[2]
    mlp_dim = wup.shape[2]
    me = lax.axis_index('sp')

    params = [pltpu.make_async_copy(src, dst, p_sem.at[i]) for i, (src, dst) in enumerate((
        (g1_hbm, g1), (s1_hbm, s1), (bqkv_hbm, bqkv), (bout_hbm, bout), (g2_hbm, g2), (s2_hbm, s2), (bup_hbm, bup), (bdown_hbm, bdown)))]

    def weight_copies(layer):
        return [pltpu.make_async_copy(src.at[layer], dst.at[layer], w_sem.at[layer, i]) for i, (src, dst) in enumerate((
            (wqkv_hbm, wqkv), (wout_hbm, wout), (wup_hbm, wup), (wdown_hbm, wdown)))]

    my_rows = pl.ds(pl.multiple_of(me * block, block), block)

    def send_in(image, ask):
        for core in range(2):
            for parity in range(2):
                odd = lax.rem(me // 2 + parity, 2)
                for even_hop, odd_hop in zip(hops(peers, 0), hops(peers, 1)):
                    peer = 2 * lax.rem(me // 2 + even_hop + odd * (odd_hop - even_hop), peers // 2) + core

                    if ask:
                        @pl.when(peer > me)
                        def _():
                            pl.semaphore_wait(ready.at[peer], 1)

                    @pl.when(peer != me)
                    def _():
                        pltpu.make_async_remote_copy(
                            src_ref=x_ref.at[peer * images + image], dst_ref=hid.at[image, my_rows, :],
                            send_sem=in_send, recv_sem=in_recv.at[image],
                            device_id={'sp': peer}, device_id_type=MESH).start()
        pltpu.make_async_copy(x_ref.at[me * images + image], hid.at[image, my_rows, :], in_recv.at[image]).start()

    for copy in params:
        copy.start()
    for copy in weight_copies(0):
        copy.start()

    barrier = pltpu.get_barrier_semaphore()

    @pl.loop(me + 1, peers)
    def _(peer):
        pl.semaphore_signal(barrier, inc=1, device_id={'sp': peer}, device_id_type=MESH)

    @pl.when(me > 0)
    def _():
        pl.semaphore_wait(barrier, me)

    @pl.loop(0, me)
    def _(peer):
        pl.semaphore_signal(ready.at[me], inc=1, device_id={'sp': peer}, device_id_type=MESH)

    send_in(0, True)
    for layer in range(1, layers):
        for copy in weight_copies(layer):
            copy.start()
    for copy in params:
        copy.wait()

    def body(step_idx):
        last = isinstance(step_idx, int)
        image = step_idx // layers
        layer = step_idx % layers if last else lax.rem(step_idx, layers)
        state = hid.at[image]

        @when(image == 0)
        def _():
            for copy in weight_copies(layer)[:2]:
                copy.wait()

        @when(layer == 0)
        def _():
            pltpu.make_async_copy(state, state, in_recv.at[image]).wait()

        row = pl.ds(layer, 1)
        norm_rows(state, normed, g1[row, :], s1[row, :], 32)

        group = 256
        group_heads = group // head_dim
        bias_q, bias_v = bqkv[layer, 0].T, bqkv[layer, 2].T

        def make_rows(slot, bias, dst, index):
            start = index * group
            part = lax.dot_general(wqkv[layer, pl.ds(slot * width + start, group), :], normed[...], NT, preferred_element_type=F32)
            for off in range(0, group, head_dim):
                head = (start + off) // head_dim
                dst[pl.ds(start + off, head_dim), :] = (part[off:off + head_dim] + bias[:, head:head + 1]).astype(BF)

        def make_keys(index):
            start = index * group
            part = lax.dot_general(normed[...], wqkv[layer, pl.ds(width + start, group), :], NT, preferred_element_type=F32)
            bias = jnp.concatenate([bqkv[layer, 1, pl.ds((start + off) // head_dim, 1), :] for off in range(0, group, head_dim)], axis=-1)
            keys[:, pl.ds(start, group)] = (part + bias).astype(BF)

        scale = head_dim ** -0.5 / math.log(2.0)
        zeros = jnp.zeros((head_dim, tokens), BF)

        def score(head):
            pair = head // 2 * 2
            q_head = q_t[pl.ds(head * head_dim, head_dim), :]
            rhs = jnp.concatenate([q_head, zeros] if head == pair else [zeros, q_head], axis=0)
            part = jnp.dot(keys[:, pl.ds(pair * head_dim, 2 * head_dim)], rhs, preferred_element_type=F32)
            scores[head % 4] = part
            peaks[head % 4] = jnp.max(part, axis=0, keepdims=True)

        def soften(head):
            prob = jnp.exp2((scores[head % 4] - peaks[head % 4]) * scale)
            totals[head % 4] = jnp.sum(prob, axis=0, keepdims=True)
            probs[head % 4] = prob.astype(BF)

        def mix(head):
            part = jnp.dot(v_t[pl.ds(head * head_dim, head_dim), :], probs[head % 4], preferred_element_type=F32)
            mixed_t[pl.ds(head * head_dim, head_dim), :] = part * (1.0 / totals[head % 4])

        make_rows(0, bias_q, q_t, 0)
        make_keys(0)
        make_rows(2, bias_v, v_t, 0)
        for step in range(0, heads + 4, 2):
            for head in (step, step + 1):
                if head < heads:
                    score(head)
            ahead = step // group_heads + 1
            if ahead * group < width:
                if step % group_heads == 0:
                    make_rows(0, bias_q, q_t, ahead)
                    make_keys(ahead)
                else:
                    make_rows(2, bias_v, v_t, ahead)
            for head in (step - 2, step - 1):
                if 0 <= head < heads:
                    soften(head)
            for head in (step - 4, step - 3):
                if 0 <= head < heads:
                    mix(head)
            if step >= 4:
                cols = pl.ds((step - 4) * head_dim, 2 * head_dim)
                mixed[:, cols] = mixed_t[cols, :].T.astype(BF)

        for start in range(0, width, 512):
            cols = pl.ds(start, 512)
            part = jnp.dot(mixed[...], wout[layer, :, cols], preferred_element_type=F32) + bout[row, cols]
            state[:, cols] = (state[:, cols].astype(F32) + part).astype(BF)

        @when(image == 0)
        def _():
            for copy in weight_copies(layer)[2:]:
                copy.wait()

        @when(step_idx == 0)
        def _():
            for other in range(1, images):
                send_in(other, False)

        slot = me * images + image

        def give(peer):
            rows = pl.ds(peer * block, block) if isinstance(peer, int) else pl.ds(pl.multiple_of(peer * block, block), block)
            pltpu.make_async_remote_copy(
                src_ref=hid.at[image, rows, :], dst_ref=out_ref.at[slot],
                send_sem=out_send, recv_sem=out_recv,
                device_id={'sp': peer}, device_id_type=MESH).start()

        def leave():
            for peer in (1, 0):
                @pl.when(peer != me)
                def _():
                    give(peer)

            for hop in sorted(range(peers // 2), key=lambda hop: (-min(hop, peers // 2 - hop), hop)):
                for core in range(2):
                    peer = 2 * lax.rem(me // 2 + hop, peers // 2) + core

                    @pl.when(jnp.logical_and(peer != me, peer > 1))
                    def _():
                        give(peer)

            out_ref[slot] = hid[image, my_rows, :]

        chip_rows = 2 * block
        chips = peers // 2
        early = (0, chips - 2) + tuple(range(1, chips // 2 - 1))
        parts = (early, (chips // 2 - 1,) + tuple(chip for chip in reversed(range(chips)) if chip not in early + (chips // 2 - 1,)))

        def leave_part(part):
            for chip in parts[part]:
                for core in range(2):
                    peer = 2 * chip + core

                    @pl.when(peer != me)
                    def _():
                        give(peer)

                    @pl.when(peer == me)
                    def _():
                        out_ref[slot] = hid[image, my_rows, :]

        if last:
            half = tokens // 2

            def norm_part(part):
                for index, chip in enumerate(parts[part]):
                    norm_rows(state.at[pl.ds(chip * chip_rows, chip_rows), :],
                              normed.at[pl.ds(part * half + index * chip_rows, chip_rows), :], g2[row, :], s2[row, :], 32)

            def widen_part(part):
                rows = pl.ds(part * half, half)
                for start in range(0, mlp_dim, 512):
                    cols = pl.ds(start, 512)
                    part_up = jnp.dot(normed[rows, :], wup[layer, :, cols], preferred_element_type=F32) + bup[row, cols]
                    active[rows, cols] = gelu(part_up).astype(BF)

            def narrow_part(part):
                for start in range(0, width, 512):
                    cols = pl.ds(start, 512)
                    part_down = jnp.dot(active[pl.ds(part * half, half), :], wdown[layer, :, cols], preferred_element_type=F32) + bdown[row, cols]
                    for index, chip in enumerate(parts[part]):
                        rows = pl.ds(chip * chip_rows, chip_rows)
                        state[rows, cols] = (state[rows, cols].astype(F32) + part_down[index * chip_rows:(index + 1) * chip_rows]).astype(BF)

            norm_part(0)
            widen_part(0)
            norm_part(1)
            narrow_part(0)
            leave_part(0)
            widen_part(1)
            narrow_part(1)
            leave_part(1)
        else:
            norm_rows(state, normed, g2[row, :], s2[row, :], 32)
            for start in range(0, mlp_dim, 512):
                cols = pl.ds(start, 512)
                part = jnp.dot(normed[...], wup[layer, :, cols], preferred_element_type=F32) + bup[row, cols]
                active[:, cols] = gelu(part).astype(BF)
            for start in range(0, width, 512):
                cols = pl.ds(start, 512)
                part = jnp.dot(active[...], wdown[layer, :, cols], preferred_element_type=F32) + bdown[row, cols]
                state[:, cols] = (state[:, cols].astype(F32) + part).astype(BF)

            pl.when(layer == layers - 1)(leave)

    @pl.loop(0, images * layers - 1)
    def _(step_idx):
        body(step_idx)

    body(images * layers - 1)

    sent = x_ref.at[pl.ds(0, (peers - 1) * images)]
    pltpu.make_async_copy(sent, sent, in_send).wait()
    pltpu.make_async_copy(sent, sent, out_send).wait()
    pltpu.make_async_copy(sent, sent, out_recv).wait()


def solution(mesh):
    token_spec = P('dp', 'sp', None)
    peers = mesh.shape['sp']

    def device_step(image_tokens, ln1_gain, ln1_shift, w_qkv, b_qkv, w_out, b_out, ln2_gain, ln2_shift, w_up, b_up, w_down, b_down):
        total_images, block, width = image_tokens.shape
        layers, _, _, heads, head_dim = w_qkv.shape
        mlp_dim = w_up.shape[-1]
        images = total_images // peers
        tokens = block * peers
        inner = heads * head_dim
        w_qkv_t = jnp.transpose(w_qkv, (0, 2, 3, 4, 1)).reshape(layers, 3 * inner, width)
        w_out_m = w_out.reshape(layers, inner, width)
        args = (image_tokens, ln1_gain, ln1_shift, w_qkv_t, b_qkv, w_out_m, b_out, ln2_gain, ln2_shift, w_up, b_up, w_down, b_down)
        small = lambda a: pltpu.VMEM(a.shape, a.dtype)
        return pl.pallas_call(
            functools.partial(kernel, peers),
            out_shape=pltpu.VMEM(image_tokens.shape, image_tokens.dtype),
            in_specs=[pl.BlockSpec(memory_space=pl.ANY)] * len(args),
            out_specs=pl.BlockSpec(memory_space=pltpu.VMEM),
            scratch_shapes=[
                pltpu.VMEM((images, tokens, width), BF),
                small(w_qkv_t), small(w_out_m), small(w_up), small(w_down),
                small(ln1_gain), small(ln1_shift), small(b_qkv), small(b_out), small(ln2_gain), small(ln2_shift), small(b_up), small(b_down),
                pltpu.VMEM((tokens, width), BF),
                pltpu.VMEM((inner, tokens), BF),
                pltpu.VMEM((inner, tokens), BF),
                pltpu.VMEM((tokens, inner), BF),
                pltpu.VMEM((tokens, inner), BF),
                pltpu.VMEM((tokens, mlp_dim), BF),
                pltpu.VMEM((4, tokens, tokens), F32),
                pltpu.VMEM((4, tokens, tokens), BF),
                pltpu.VMEM((4, 1, tokens), F32),
                pltpu.VMEM((4, 1, tokens), F32),
                pltpu.VMEM((inner, tokens), F32),
                pltpu.SemaphoreType.REGULAR((peers,)),
                pltpu.SemaphoreType.DMA((layers, 4)),
                pltpu.SemaphoreType.DMA((8,)),
                pltpu.SemaphoreType.DMA,
                pltpu.SemaphoreType.DMA((images,)),
                pltpu.SemaphoreType.DMA,
                pltpu.SemaphoreType.DMA,
            ],
            compiler_params=pltpu.CompilerParams(collective_id=0, has_side_effects=True, vmem_limit_bytes=65_500_000),
        )(*args)

    return jax.shard_map(device_step, mesh=mesh, in_specs=(token_spec,) + (P(),) * 12, out_specs=token_spec, check_vma=False)
```

```python
import functools
import math

import jax
import jax.numpy as jnp
from jax import lax
from jax.experimental import pallas as pl
from jax.experimental.pallas import tpu as pltpu
from jax.sharding import PartitionSpec as P

LN_EPS = 1e-6
MESH = pl.DeviceIdType.MESH
BF = jnp.bfloat16
F32 = jnp.float32
NT = (((1,), (1,)), ((), ()))


def norm_rows(src, dst, gain, shift, rows):
    total = src.shape[0]
    width = src.shape[1]
    for start in range(0, total, rows):
        values = src[pl.ds(start, rows), :].astype(F32)
        mean_val = jnp.sum(values, axis=-1, keepdims=True) * (1.0 / width)
        centred = values - mean_val
        var_val = jnp.sum(centred * centred, axis=-1, keepdims=True) * (1.0 / width)
        dst[pl.ds(start, rows), :] = (centred * lax.rsqrt(var_val + LN_EPS) * gain + shift).astype(BF)


def gelu(x):
    c0 = math.sqrt(2.0 / math.pi)
    c1 = c0 * 0.044715
    return 0.5 * x * (1.0 + jnp.tanh(x * (c0 + c1 * (x * x))))


def hops(peers, parity):
    chips = peers // 2
    return sorted(range(parity, chips, 2), key=lambda hop: (-min(hop, chips - hop), hop))


def when(cond):
    if isinstance(cond, bool):
        return (lambda run: run()) if cond else (lambda run: None)
    return pl.when(cond)


def kernel(peers, x_ref, g1_hbm, s1_hbm, wqkv_hbm, bqkv_hbm, wout_hbm, bout_hbm, g2_hbm, s2_hbm, wup_hbm, bup_hbm, wdown_hbm, bdown_hbm,
           out_ref,
           hid, wqkv, wout, wup, wdown, g1, s1, bqkv, bout, g2, s2, bup, bdown,
           normed, q_t, v_t, keys, mixed, active, scores, probs, peaks, totals, mixed_t,
           ready, w_sem, p_sem, in_send, in_recv, out_send, out_recv):
    images = hid.shape[0]
    block = x_ref.shape[1]
    layers, heads, head_dim = bqkv.shape[0], bqkv.shape[2], bqkv.shape[3]
    tokens, width = hid.shape[1], hid.shape[2]
    mlp_dim = wup.shape[2]
    me = lax.axis_index('sp')

    params = [pltpu.make_async_copy(src, dst, p_sem.at[i]) for i, (src, dst) in enumerate((
        (g1_hbm, g1), (s1_hbm, s1), (bqkv_hbm, bqkv), (bout_hbm, bout), (g2_hbm, g2), (s2_hbm, s2), (bup_hbm, bup), (bdown_hbm, bdown)))]

    def weight_copies(layer):
        return [pltpu.make_async_copy(src.at[layer], dst.at[layer], w_sem.at[layer, i]) for i, (src, dst) in enumerate((
            (wqkv_hbm, wqkv), (wout_hbm, wout), (wup_hbm, wup), (wdown_hbm, wdown)))]

    my_rows = pl.ds(pl.multiple_of(me * block, block), block)

    def send_in(image, ask):
        for core in range(2):
            for parity in range(2):
                odd = lax.rem(me // 2 + parity, 2)
                for even_hop, odd_hop in zip(hops(peers, 0), hops(peers, 1)):
                    peer = 2 * lax.rem(me // 2 + even_hop + odd * (odd_hop - even_hop), peers // 2) + core

                    if ask:
                        @pl.when(peer > me)
                        def _():
                            pl.semaphore_wait(ready.at[peer], 1)

                    @pl.when(peer != me)
                    def _():
                        pltpu.make_async_remote_copy(
                            src_ref=x_ref.at[peer * images + image], dst_ref=hid.at[image, my_rows, :],
                            send_sem=in_send, recv_sem=in_recv.at[image],
                            device_id={'sp': peer}, device_id_type=MESH).start()
        pltpu.make_async_copy(x_ref.at[me * images + image], hid.at[image, my_rows, :], in_recv.at[image]).start()

    for copy in params:
        copy.start()
    for copy in weight_copies(0):
        copy.start()

    barrier = pltpu.get_barrier_semaphore()

    @pl.loop(me + 1, peers)
    def _(peer):
        pl.semaphore_signal(barrier, inc=1, device_id={'sp': peer}, device_id_type=MESH)

    @pl.when(me > 0)
    def _():
        pl.semaphore_wait(barrier, me)

    @pl.loop(0, me)
    def _(peer):
        pl.semaphore_signal(ready.at[me], inc=1, device_id={'sp': peer}, device_id_type=MESH)

    send_in(0, True)
    for layer in range(1, layers):
        for copy in weight_copies(layer):
            copy.start()
    for copy in params:
        copy.wait()

    def body(step_idx):
        last = isinstance(step_idx, int)
        image = step_idx // layers
        layer = step_idx % layers if last else lax.rem(step_idx, layers)
        state = hid.at[image]

        @when(image == 0)
        def _():
            for copy in weight_copies(layer)[:2]:
                copy.wait()

        @when(layer == 0)
        def _():
            pltpu.make_async_copy(state, state, in_recv.at[image]).wait()

        row = pl.ds(layer, 1)
        norm_rows(state, normed, g1[row, :], s1[row, :], 32)

        group = 256
        group_heads = group // head_dim
        bias_q, bias_v = bqkv[layer, 0].T, bqkv[layer, 2].T

        def make_rows(slot, bias, dst, index):
            start = index * group
            part = lax.dot_general(wqkv[layer, pl.ds(slot * width + start, group), :], normed[...], NT, preferred_element_type=F32)
            for off in range(0, group, head_dim):
                head = (start + off) // head_dim
                dst[pl.ds(start + off, head_dim), :] = (part[off:off + head_dim] + bias[:, head:head + 1]).astype(BF)

        def make_keys(index):
            start = index * group
            part = lax.dot_general(normed[...], wqkv[layer, pl.ds(width + start, group), :], NT, preferred_element_type=F32)
            bias = jnp.concatenate([bqkv[layer, 1, pl.ds((start + off) // head_dim, 1), :] for off in range(0, group, head_dim)], axis=-1)
            keys[:, pl.ds(start, group)] = (part + bias).astype(BF)

        scale = head_dim ** -0.5 / math.log(2.0)
        zeros = jnp.zeros((head_dim, tokens), BF)

        def score(head):
            pair = head // 2 * 2
            q_head = q_t[pl.ds(head * head_dim, head_dim), :]
            rhs = jnp.concatenate([q_head, zeros] if head == pair else [zeros, q_head], axis=0)
            part = jnp.dot(keys[:, pl.ds(pair * head_dim, 2 * head_dim)], rhs, preferred_element_type=F32)
            scores[head % 4] = part
            peaks[head % 4] = jnp.max(part, axis=0, keepdims=True)

        def soften(head):
            prob = jnp.exp2((scores[head % 4] - peaks[head % 4]) * scale)
            totals[head % 4] = jnp.sum(prob, axis=0, keepdims=True)
            probs[head % 4] = prob.astype(BF)

        def mix(head):
            part = jnp.dot(v_t[pl.ds(head * head_dim, head_dim), :], probs[head % 4], preferred_element_type=F32)
            mixed_t[pl.ds(head * head_dim, head_dim), :] = part * (1.0 / totals[head % 4])

        make_rows(0, bias_q, q_t, 0)
        make_keys(0)
        make_rows(2, bias_v, v_t, 0)
        for step in range(0, heads + 4, 2):
            for head in (step, step + 1):
                if head < heads:
                    score(head)
            ahead = step // group_heads + 1
            if ahead * group < width:
                if step % group_heads == 0:
                    make_rows(0, bias_q, q_t, ahead)
                    make_keys(ahead)
                else:
                    make_rows(2, bias_v, v_t, ahead)
            for head in (step - 2, step - 1):
                if 0 <= head < heads:
                    soften(head)
            for head in (step - 4, step - 3):
                if 0 <= head < heads:
                    mix(head)
            if step >= 4:
                cols = pl.ds((step - 4) * head_dim, 2 * head_dim)
                mixed[:, cols] = mixed_t[cols, :].T.astype(BF)

        for start in range(0, width, 512):
            cols = pl.ds(start, 512)
            part = jnp.dot(mixed[...], wout[layer, :, cols], preferred_element_type=F32) + bout[row, cols]
            state[:, cols] = (state[:, cols].astype(F32) + part).astype(BF)

        @when(image == 0)
        def _():
            for copy in weight_copies(layer)[2:]:
                copy.wait()

        @when(step_idx == 0)
        def _():
            for other in range(1, images):
                send_in(other, False)

        slot = me * images + image

        def give(peer):
            rows = pl.ds(peer * block, block) if isinstance(peer, int) else pl.ds(pl.multiple_of(peer * block, block), block)
            pltpu.make_async_remote_copy(
                src_ref=hid.at[image, rows, :], dst_ref=out_ref.at[slot],
                send_sem=out_send, recv_sem=out_recv,
                device_id={'sp': peer}, device_id_type=MESH).start()

        def leave():
            for peer in (1, 0):
                @pl.when(peer != me)
                def _():
                    give(peer)

            for hop in sorted(range(peers // 2), key=lambda hop: (-min(hop, peers // 2 - hop), hop)):
                for core in range(2):
                    peer = 2 * lax.rem(me // 2 + hop, peers // 2) + core

                    @pl.when(jnp.logical_and(peer != me, peer > 1))
                    def _():
                        give(peer)

            out_ref[slot] = hid[image, my_rows, :]

        chip_rows = 2 * block
        chips = peers // 2
        early = tuple(range(chips // 2 - 1)) + (chips - 2,)
        parts = (early, (chips // 2 - 1,) + tuple(chip for chip in reversed(range(chips)) if chip not in early + (chips // 2 - 1,)))

        def leave_part(part):
            for chip in parts[part]:
                for core in (1, 0):
                    peer = 2 * chip + core

                    @pl.when(peer != me)
                    def _():
                        give(peer)

                    @pl.when(peer == me)
                    def _():
                        out_ref[slot] = hid[image, my_rows, :]

        if last:
            half = tokens // 2

            def norm_part(part):
                for index, chip in enumerate(parts[part]):
                    norm_rows(state.at[pl.ds(chip * chip_rows, chip_rows), :],
                              normed.at[pl.ds(part * half + index * chip_rows, chip_rows), :], g2[row, :], s2[row, :], 32)

            def widen_part(part):
                rows = pl.ds(part * half, half)
                for start in range(0, mlp_dim, 512):
                    cols = pl.ds(start, 512)
                    part_up = jnp.dot(normed[rows, :], wup[layer, :, cols], preferred_element_type=F32) + bup[row, cols]
                    active[rows, cols] = gelu(part_up).astype(BF)

            def narrow_part(part):
                for start in range(0, width, 512):
                    cols = pl.ds(start, 512)
                    part_down = jnp.dot(active[pl.ds(part * half, half), :], wdown[layer, :, cols], preferred_element_type=F32) + bdown[row, cols]
                    for index, chip in enumerate(parts[part]):
                        rows = pl.ds(chip * chip_rows, chip_rows)
                        state[rows, cols] = (state[rows, cols].astype(F32) + part_down[index * chip_rows:(index + 1) * chip_rows]).astype(BF)

            norm_part(0)
            widen_part(0)
            norm_part(1)
            narrow_part(0)
            leave_part(0)
            widen_part(1)
            narrow_part(1)
            leave_part(1)
        else:
            norm_rows(state, normed, g2[row, :], s2[row, :], 32)
            for start in range(0, mlp_dim, 512):
                cols = pl.ds(start, 512)
                part = jnp.dot(normed[...], wup[layer, :, cols], preferred_element_type=F32) + bup[row, cols]
                active[:, cols] = gelu(part).astype(BF)
            for start in range(0, width, 512):
                cols = pl.ds(start, 512)
                part = jnp.dot(active[...], wdown[layer, :, cols], preferred_element_type=F32) + bdown[row, cols]
                state[:, cols] = (state[:, cols].astype(F32) + part).astype(BF)

            pl.when(layer == layers - 1)(leave)

    @pl.loop(0, images * layers - 1)
    def _(step_idx):
        body(step_idx)

    body(images * layers - 1)

    sent = x_ref.at[pl.ds(0, (peers - 1) * images)]
    pltpu.make_async_copy(sent, sent, in_send).wait()
    pltpu.make_async_copy(sent, sent, out_send).wait()
    pltpu.make_async_copy(sent, sent, out_recv).wait()


def solution(mesh):
    token_spec = P('dp', 'sp', None)
    peers = mesh.shape['sp']

    def device_step(image_tokens, ln1_gain, ln1_shift, w_qkv, b_qkv, w_out, b_out, ln2_gain, ln2_shift, w_up, b_up, w_down, b_down):
        total_images, block, width = image_tokens.shape
        layers, _, _, heads, head_dim = w_qkv.shape
        mlp_dim = w_up.shape[-1]
        images = total_images // peers
        tokens = block * peers
        inner = heads * head_dim
        w_qkv_t = jnp.transpose(w_qkv, (0, 2, 3, 4, 1)).reshape(layers, 3 * inner, width)
        w_out_m = w_out.reshape(layers, inner, width)
        args = (image_tokens, ln1_gain, ln1_shift, w_qkv_t, b_qkv, w_out_m, b_out, ln2_gain, ln2_shift, w_up, b_up, w_down, b_down)
        small = lambda a: pltpu.VMEM(a.shape, a.dtype)
        return pl.pallas_call(
            functools.partial(kernel, peers),
            out_shape=pltpu.VMEM(image_tokens.shape, image_tokens.dtype),
            in_specs=[pl.BlockSpec(memory_space=pl.ANY)] * len(args),
            out_specs=pl.BlockSpec(memory_space=pltpu.VMEM),
            scratch_shapes=[
                pltpu.VMEM((images, tokens, width), BF),
                small(w_qkv_t), small(w_out_m), small(w_up), small(w_down),
                small(ln1_gain), small(ln1_shift), small(b_qkv), small(b_out), small(ln2_gain), small(ln2_shift), small(b_up), small(b_down),
                pltpu.VMEM((tokens, width), BF),
                pltpu.VMEM((inner, tokens), BF),
                pltpu.VMEM((inner, tokens), BF),
                pltpu.VMEM((tokens, inner), BF),
                pltpu.VMEM((tokens, inner), BF),
                pltpu.VMEM((tokens, mlp_dim), BF),
                pltpu.VMEM((4, tokens, tokens), F32),
                pltpu.VMEM((4, tokens, tokens), BF),
                pltpu.VMEM((4, 1, tokens), F32),
                pltpu.VMEM((4, 1, tokens), F32),
                pltpu.VMEM((inner, tokens), F32),
                pltpu.SemaphoreType.REGULAR((peers,)),
                pltpu.SemaphoreType.DMA((layers, 4)),
                pltpu.SemaphoreType.DMA((8,)),
                pltpu.SemaphoreType.DMA,
                pltpu.SemaphoreType.DMA((images,)),
                pltpu.SemaphoreType.DMA,
                pltpu.SemaphoreType.DMA,
            ],
            compiler_params=pltpu.CompilerParams(collective_id=0, has_side_effects=True, vmem_limit_bytes=65_500_000),
        )(*args)

    return jax.shard_map(device_step, mesh=mesh, in_specs=(token_spec,) + (P(),) * 12, out_specs=token_spec, check_vma=False)
```

```python
import functools
import math

import jax
import jax.numpy as jnp
from jax import lax
from jax.experimental import pallas as pl
from jax.experimental.pallas import tpu as pltpu
from jax.sharding import PartitionSpec as P

LN_EPS = 1e-6
MESH = pl.DeviceIdType.MESH
BF = jnp.bfloat16
F32 = jnp.float32
NT = (((1,), (1,)), ((), ()))


def norm_rows(src, dst, gain, shift, rows):
    total = src.shape[0]
    width = src.shape[1]
    for start in range(0, total, rows):
        values = src[pl.ds(start, rows), :].astype(F32)
        mean_val = jnp.sum(values, axis=-1, keepdims=True) * (1.0 / width)
        centred = values - mean_val
        var_val = jnp.sum(centred * centred, axis=-1, keepdims=True) * (1.0 / width)
        dst[pl.ds(start, rows), :] = (centred * lax.rsqrt(var_val + LN_EPS) * gain + shift).astype(BF)


def gelu(x):
    c0 = math.sqrt(2.0 / math.pi)
    c1 = c0 * 0.044715
    return 0.5 * x * (1.0 + jnp.tanh(x * (c0 + c1 * (x * x))))


def hops(peers, parity):
    chips = peers // 2
    return sorted(range(parity, chips, 2), key=lambda hop: (-min(hop, chips - hop), hop))


def when(cond):
    if isinstance(cond, bool):
        return (lambda run: run()) if cond else (lambda run: None)
    return pl.when(cond)


def kernel(peers, x_ref, g1_hbm, s1_hbm, wqkv_hbm, bqkv_hbm, wout_hbm, bout_hbm, g2_hbm, s2_hbm, wup_hbm, bup_hbm, wdown_hbm, bdown_hbm,
           out_ref,
           hid, wqkv, wout, wup, wdown, g1, s1, bqkv, bout, g2, s2, bup, bdown,
           normed, q_t, v_t, keys, mixed, active, scores, probs, peaks, totals, mixed_t,
           ready, w_sem, p_sem, in_send, in_recv, out_send, out_recv):
    images = hid.shape[0]
    block = x_ref.shape[1]
    layers, heads, head_dim = bqkv.shape[0], bqkv.shape[2], bqkv.shape[3]
    tokens, width = hid.shape[1], hid.shape[2]
    mlp_dim = wup.shape[2]
    me = lax.axis_index('sp')

    params = [pltpu.make_async_copy(src, dst, p_sem.at[i]) for i, (src, dst) in enumerate((
        (g1_hbm, g1), (s1_hbm, s1), (bqkv_hbm, bqkv), (bout_hbm, bout), (g2_hbm, g2), (s2_hbm, s2), (bup_hbm, bup), (bdown_hbm, bdown)))]

    def weight_copies(layer):
        return [pltpu.make_async_copy(src.at[layer], dst.at[layer], w_sem.at[layer, i]) for i, (src, dst) in enumerate((
            (wqkv_hbm, wqkv), (wout_hbm, wout), (wup_hbm, wup), (wdown_hbm, wdown)))]

    my_rows = pl.ds(pl.multiple_of(me * block, block), block)

    def send_in(image, ask):
        for core in range(2):
            for parity in range(2):
                odd = lax.rem(me // 2 + parity, 2)
                for even_hop, odd_hop in zip(hops(peers, 0), hops(peers, 1)):
                    peer = 2 * lax.rem(me // 2 + even_hop + odd * (odd_hop - even_hop), peers // 2) + core

                    if ask:
                        @pl.when(peer > me)
                        def _():
                            pl.semaphore_wait(ready.at[peer], 1)

                    @pl.when(peer != me)
                    def _():
                        pltpu.make_async_remote_copy(
                            src_ref=x_ref.at[peer * images + image], dst_ref=hid.at[image, my_rows, :],
                            send_sem=in_send, recv_sem=in_recv.at[image],
                            device_id={'sp': peer}, device_id_type=MESH).start()
        pltpu.make_async_copy(x_ref.at[me * images + image], hid.at[image, my_rows, :], in_recv.at[image]).start()

    for copy in params:
        copy.start()
    for copy in weight_copies(0):
        copy.start()

    barrier = pltpu.get_barrier_semaphore()

    @pl.loop(me + 1, peers)
    def _(peer):
        pl.semaphore_signal(barrier, inc=1, device_id={'sp': peer}, device_id_type=MESH)

    @pl.when(me > 0)
    def _():
        pl.semaphore_wait(barrier, me)

    @pl.loop(0, me)
    def _(peer):
        pl.semaphore_signal(ready.at[me], inc=1, device_id={'sp': peer}, device_id_type=MESH)

    send_in(0, True)
    for layer in range(1, layers):
        for copy in weight_copies(layer):
            copy.start()
    for copy in params:
        copy.wait()

    def body(step_idx):
        last = isinstance(step_idx, int)
        image = step_idx // layers
        layer = step_idx % layers if last else lax.rem(step_idx, layers)
        state = hid.at[image]

        @when(image == 0)
        def _():
            for copy in weight_copies(layer):
                copy.wait()

        @when(layer == 0)
        def _():
            pltpu.make_async_copy(state, state, in_recv.at[image]).wait()

        final_wave = lax.rem(me, 4) == 3

        @when(False if last else jnp.logical_or(jnp.logical_and(step_idx == 0, final_wave), jnp.logical_and(step_idx == 1, jnp.logical_not(final_wave))))
        def _():
            for other in range(1, images):
                send_in(other, False)

        row = pl.ds(layer, 1)
        norm_rows(state, normed, g1[row, :], s1[row, :], 32)

        group = 256
        group_heads = group // head_dim
        bias_q, bias_v = bqkv[layer, 0].T, bqkv[layer, 2].T

        def make_rows(slot, bias, dst, index):
            start = index * group
            part = lax.dot_general(wqkv[layer, pl.ds(slot * width + start, group), :], normed[...], NT, preferred_element_type=F32)
            for off in range(0, group, head_dim):
                head = (start + off) // head_dim
                dst[pl.ds(start + off, head_dim), :] = (part[off:off + head_dim] + bias[:, head:head + 1]).astype(BF)

        def make_keys(index):
            start = index * group
            part = lax.dot_general(normed[...], wqkv[layer, pl.ds(width + start, group), :], NT, preferred_element_type=F32)
            bias = jnp.concatenate([bqkv[layer, 1, pl.ds((start + off) // head_dim, 1), :] for off in range(0, group, head_dim)], axis=-1)
            keys[:, pl.ds(start, group)] = (part + bias).astype(BF)

        scale = head_dim ** -0.5 / math.log(2.0)
        zeros = jnp.zeros((head_dim, tokens), BF)

        def score(head):
            pair = head // 2 * 2
            q_head = q_t[pl.ds(head * head_dim, head_dim), :]
            rhs = jnp.concatenate([q_head, zeros] if head == pair else [zeros, q_head], axis=0)
            part = jnp.dot(keys[:, pl.ds(pair * head_dim, 2 * head_dim)], rhs, preferred_element_type=F32)
            scores[head % 4] = part
            peaks[head % 4] = jnp.max(part, axis=0, keepdims=True)

        def soften(head):
            prob = jnp.exp2((scores[head % 4] - peaks[head % 4]) * scale)
            totals[head % 4] = jnp.sum(prob, axis=0, keepdims=True)
            probs[head % 4] = prob.astype(BF)

        def mix(head):
            part = jnp.dot(v_t[pl.ds(head * head_dim, head_dim), :], probs[head % 4], preferred_element_type=F32)
            mixed_t[pl.ds(head * head_dim, head_dim), :] = part * (1.0 / totals[head % 4])

        make_rows(0, bias_q, q_t, 0)
        make_keys(0)
        make_rows(2, bias_v, v_t, 0)
        for step in range(0, heads + 4, 2):
            for head in (step, step + 1):
                if head < heads:
                    score(head)
            ahead = step // group_heads + 1
            if ahead * group < width:
                if step % group_heads == 0:
                    make_rows(0, bias_q, q_t, ahead)
                    make_keys(ahead)
                else:
                    make_rows(2, bias_v, v_t, ahead)
            for head in (step - 2, step - 1):
                if 0 <= head < heads:
                    soften(head)
            for head in (step - 4, step - 3):
                if 0 <= head < heads:
                    mix(head)
            if step >= 4:
                cols = pl.ds((step - 4) * head_dim, 2 * head_dim)
                mixed[:, cols] = mixed_t[cols, :].T.astype(BF)

        for start in range(0, width, 512):
            cols = pl.ds(start, 512)
            part = jnp.dot(mixed[...], wout[layer, :, cols], preferred_element_type=F32) + bout[row, cols]
            state[:, cols] = (state[:, cols].astype(F32) + part).astype(BF)

        slot = me * images + image

        def give(peer):
            rows = pl.ds(peer * block, block) if isinstance(peer, int) else pl.ds(pl.multiple_of(peer * block, block), block)
            pltpu.make_async_remote_copy(
                src_ref=hid.at[image, rows, :], dst_ref=out_ref.at[slot],
                send_sem=out_send, recv_sem=out_recv,
                device_id={'sp': peer}, device_id_type=MESH).start()

        def leave():
            for peer in (1, 0):
                @pl.when(peer != me)
                def _():
                    give(peer)

            for hop in sorted(range(peers // 2), key=lambda hop: (-min(hop, peers // 2 - hop), hop)):
                for core in range(2):
                    peer = 2 * lax.rem(me // 2 + hop, peers // 2) + core

                    @pl.when(jnp.logical_and(peer != me, peer > 1))
                    def _():
                        give(peer)

            out_ref[slot] = hid[image, my_rows, :]

        chip_rows = 2 * block
        chips = peers // 2
        early = tuple(range(chips // 2 - 1)) + (chips - 2,)
        parts = (early, (chips // 2 - 1,) + tuple(chip for chip in reversed(range(chips)) if chip not in early + (chips // 2 - 1,)))

        def leave_part(part):
            for chip in parts[part]:
                for core in (1, 0):
                    peer = 2 * chip + core

                    @pl.when(peer != me)
                    def _():
                        give(peer)

                    @pl.when(peer == me)
                    def _():
                        out_ref[slot] = hid[image, my_rows, :]

        if last:
            half = tokens // 2

            def norm_part(part):
                for index, chip in enumerate(parts[part]):
                    norm_rows(state.at[pl.ds(chip * chip_rows, chip_rows), :],
                              normed.at[pl.ds(part * half + index * chip_rows, chip_rows), :], g2[row, :], s2[row, :], 32)

            def widen_part(part):
                rows = pl.ds(part * half, half)
                for start in range(0, mlp_dim, 512):
                    cols = pl.ds(start, 512)
                    part_up = jnp.dot(normed[rows, :], wup[layer, :, cols], preferred_element_type=F32) + bup[row, cols]
                    active[rows, cols] = gelu(part_up).astype(BF)

            def narrow_part(part):
                for start in range(0, width, 512):
                    cols = pl.ds(start, 512)
                    part_down = jnp.dot(active[pl.ds(part * half, half), :], wdown[layer, :, cols], preferred_element_type=F32) + bdown[row, cols]
                    for index, chip in enumerate(parts[part]):
                        rows = pl.ds(chip * chip_rows, chip_rows)
                        state[rows, cols] = (state[rows, cols].astype(F32) + part_down[index * chip_rows:(index + 1) * chip_rows]).astype(BF)

            norm_part(0)
            widen_part(0)
            norm_part(1)
            narrow_part(0)
            leave_part(0)
            widen_part(1)
            narrow_part(1)
            leave_part(1)
        else:
            norm_rows(state, normed, g2[row, :], s2[row, :], 32)
            for start in range(0, mlp_dim, 512):
                cols = pl.ds(start, 512)
                part = jnp.dot(normed[...], wup[layer, :, cols], preferred_element_type=F32) + bup[row, cols]
                active[:, cols] = gelu(part).astype(BF)
            for start in range(0, width, 512):
                cols = pl.ds(start, 512)
                part = jnp.dot(active[...], wdown[layer, :, cols], preferred_element_type=F32) + bdown[row, cols]
                state[:, cols] = (state[:, cols].astype(F32) + part).astype(BF)

            pl.when(layer == layers - 1)(leave)

    @pl.loop(0, images * layers - 1)
    def _(step_idx):
        body(step_idx)

    body(images * layers - 1)

    sent = x_ref.at[pl.ds(0, (peers - 1) * images)]
    pltpu.make_async_copy(sent, sent, in_send).wait()
    pltpu.make_async_copy(sent, sent, out_send).wait()
    pltpu.make_async_copy(sent, sent, out_recv).wait()


def solution(mesh):
    token_spec = P('dp', 'sp', None)
    peers = mesh.shape['sp']

    def device_step(image_tokens, ln1_gain, ln1_shift, w_qkv, b_qkv, w_out, b_out, ln2_gain, ln2_shift, w_up, b_up, w_down, b_down):
        total_images, block, width = image_tokens.shape
        layers, _, _, heads, head_dim = w_qkv.shape
        mlp_dim = w_up.shape[-1]
        images = total_images // peers
        tokens = block * peers
        inner = heads * head_dim
        w_qkv_t = jnp.transpose(w_qkv, (0, 2, 3, 4, 1)).reshape(layers, 3 * inner, width)
        w_out_m = w_out.reshape(layers, inner, width)
        args = (image_tokens, ln1_gain, ln1_shift, w_qkv_t, b_qkv, w_out_m, b_out, ln2_gain, ln2_shift, w_up, b_up, w_down, b_down)
        small = lambda a: pltpu.VMEM(a.shape, a.dtype)
        return pl.pallas_call(
            functools.partial(kernel, peers),
            out_shape=pltpu.VMEM(image_tokens.shape, image_tokens.dtype),
            in_specs=[pl.BlockSpec(memory_space=pl.ANY)] * len(args),
            out_specs=pl.BlockSpec(memory_space=pltpu.VMEM),
            scratch_shapes=[
                pltpu.VMEM((images, tokens, width), BF),
                small(w_qkv_t), small(w_out_m), small(w_up), small(w_down),
                small(ln1_gain), small(ln1_shift), small(b_qkv), small(b_out), small(ln2_gain), small(ln2_shift), small(b_up), small(b_down),
                pltpu.VMEM((tokens, width), BF),
                pltpu.VMEM((inner, tokens), BF),
                pltpu.VMEM((inner, tokens), BF),
                pltpu.VMEM((tokens, inner), BF),
                pltpu.VMEM((tokens, inner), BF),
                pltpu.VMEM((tokens, mlp_dim), BF),
                pltpu.VMEM((4, tokens, tokens), F32),
                pltpu.VMEM((4, tokens, tokens), BF),
                pltpu.VMEM((4, 1, tokens), F32),
                pltpu.VMEM((4, 1, tokens), F32),
                pltpu.VMEM((inner, tokens), F32),
                pltpu.SemaphoreType.REGULAR((peers,)),
                pltpu.SemaphoreType.DMA((layers, 4)),
                pltpu.SemaphoreType.DMA((8,)),
                pltpu.SemaphoreType.DMA,
                pltpu.SemaphoreType.DMA((images,)),
                pltpu.SemaphoreType.DMA,
                pltpu.SemaphoreType.DMA,
            ],
            compiler_params=pltpu.CompilerParams(collective_id=0, has_side_effects=True, vmem_limit_bytes=65_500_000),
        )(*args)

    return jax.shard_map(device_step, mesh=mesh, in_specs=(token_spec,) + (P(),) * 12, out_specs=token_spec, check_vma=False)
```

```python
import functools
import math

import jax
import jax.numpy as jnp
from jax import lax
from jax.experimental import pallas as pl
from jax.experimental.pallas import tpu as pltpu
from jax.sharding import PartitionSpec as P

LN_EPS = 1e-6
MESH = pl.DeviceIdType.MESH
BF = jnp.bfloat16
F32 = jnp.float32
NT = (((1,), (1,)), ((), ()))


def norm_rows(src, dst, gain, shift, rows):
    total = src.shape[0]
    width = src.shape[1]
    for start in range(0, total, rows):
        values = src[pl.ds(start, rows), :].astype(F32)
        mean_val = jnp.sum(values, axis=-1, keepdims=True) * (1.0 / width)
        centred = values - mean_val
        var_val = jnp.sum(centred * centred, axis=-1, keepdims=True) * (1.0 / width)
        dst[pl.ds(start, rows), :] = (centred * lax.rsqrt(var_val + LN_EPS) * gain + shift).astype(BF)


def gelu(x):
    c0 = math.sqrt(2.0 / math.pi)
    c1 = c0 * 0.044715
    return 0.5 * x * (1.0 + jnp.tanh(x * (c0 + c1 * (x * x))))


def hops(peers, parity):
    chips = peers // 2
    return sorted(range(parity, chips, 2), key=lambda hop: (-min(hop, chips - hop), hop))


def when(cond):
    if isinstance(cond, bool):
        return (lambda run: run()) if cond else (lambda run: None)
    return pl.when(cond)


def kernel(peers, x_ref, g1_hbm, s1_hbm, wqkv_hbm, bqkv_hbm, wout_hbm, bout_hbm, g2_hbm, s2_hbm, wup_hbm, bup_hbm, wdown_hbm, bdown_hbm,
           out_ref,
           hid, wqkv, wout, wup, wdown, g1, s1, bqkv, bout, g2, s2, bup, bdown,
           normed, q_t, v_t, keys, mixed, active, scores, probs, peaks, totals, mixed_t,
           ready, w_sem, p_sem, in_send, in_recv, out_send, out_recv):
    images = hid.shape[0]
    block = x_ref.shape[1]
    layers, heads, head_dim = bqkv.shape[0], bqkv.shape[2], bqkv.shape[3]
    tokens, width = hid.shape[1], hid.shape[2]
    mlp_dim = wup.shape[2]
    me = lax.axis_index('sp')

    params = [pltpu.make_async_copy(src, dst, p_sem.at[i]) for i, (src, dst) in enumerate((
        (g1_hbm, g1), (s1_hbm, s1), (bqkv_hbm, bqkv), (bout_hbm, bout), (g2_hbm, g2), (s2_hbm, s2), (bup_hbm, bup), (bdown_hbm, bdown)))]

    def weight_copies(layer):
        return [pltpu.make_async_copy(src.at[layer], dst.at[layer], w_sem.at[layer, i]) for i, (src, dst) in enumerate((
            (wqkv_hbm, wqkv), (wout_hbm, wout), (wup_hbm, wup), (wdown_hbm, wdown)))]

    my_rows = pl.ds(pl.multiple_of(me * block, block), block)

    def send_in(image, ask):
        for core in (1, 0):
            for parity in range(2):
                odd = lax.rem(me // 2 + parity, 2)
                for even_hop, odd_hop in zip(hops(peers, 0), hops(peers, 1)):
                    peer = 2 * lax.rem(me // 2 + even_hop + odd * (odd_hop - even_hop), peers // 2) + core

                    if ask:
                        @pl.when(peer > me)
                        def _():
                            pl.semaphore_wait(ready.at[peer], 1)

                    @pl.when(peer != me)
                    def _():
                        pltpu.make_async_remote_copy(
                            src_ref=x_ref.at[peer * images + image], dst_ref=hid.at[image, my_rows, :],
                            send_sem=in_send, recv_sem=in_recv.at[image],
                            device_id={'sp': peer}, device_id_type=MESH).start()
        pltpu.make_async_copy(x_ref.at[me * images + image], hid.at[image, my_rows, :], in_recv.at[image]).start()

    for copy in params:
        copy.start()
    for copy in weight_copies(0):
        copy.start()

    barrier = pltpu.get_barrier_semaphore()

    @pl.loop(me + 1, peers)
    def _(peer):
        pl.semaphore_signal(barrier, inc=1, device_id={'sp': peer}, device_id_type=MESH)

    @pl.when(me > 0)
    def _():
        pl.semaphore_wait(barrier, me)

    @pl.loop(0, me)
    def _(peer):
        pl.semaphore_signal(ready.at[me], inc=1, device_id={'sp': peer}, device_id_type=MESH)

    send_in(0, True)
    for layer in range(1, layers):
        for copy in weight_copies(layer):
            copy.start()
    for copy in params:
        copy.wait()

    def body(step_idx):
        last = isinstance(step_idx, int)
        image = step_idx // layers
        layer = step_idx % layers if last else lax.rem(step_idx, layers)
        state = hid.at[image]

        @when(image == 0)
        def _():
            for copy in weight_copies(layer)[:2]:
                copy.wait()

        @when(layer == 0)
        def _():
            pltpu.make_async_copy(state, state, in_recv.at[image]).wait()

        row = pl.ds(layer, 1)
        norm_rows(state, normed, g1[row, :], s1[row, :], 32)

        group = 256
        group_heads = group // head_dim
        bias_q, bias_v = bqkv[layer, 0].T, bqkv[layer, 2].T

        def make_rows(slot, bias, dst, index):
            start = index * group
            part = lax.dot_general(wqkv[layer, pl.ds(slot * width + start, group), :], normed[...], NT, preferred_element_type=F32)
            for off in range(0, group, head_dim):
                head = (start + off) // head_dim
                dst[pl.ds(start + off, head_dim), :] = (part[off:off + head_dim] + bias[:, head:head + 1]).astype(BF)

        def make_keys(index):
            start = index * group
            part = lax.dot_general(normed[...], wqkv[layer, pl.ds(width + start, group), :], NT, preferred_element_type=F32)
            bias = jnp.concatenate([bqkv[layer, 1, pl.ds((start + off) // head_dim, 1), :] for off in range(0, group, head_dim)], axis=-1)
            keys[:, pl.ds(start, group)] = (part + bias).astype(BF)

        scale = head_dim ** -0.5 / math.log(2.0)
        zeros = jnp.zeros((head_dim, tokens), BF)

        def score(head):
            pair = head // 2 * 2
            q_head = q_t[pl.ds(head * head_dim, head_dim), :]
            rhs = jnp.concatenate([q_head, zeros] if head == pair else [zeros, q_head], axis=0)
            part = jnp.dot(keys[:, pl.ds(pair * head_dim, 2 * head_dim)], rhs, preferred_element_type=F32)
            scores[head % 4] = part
            peaks[head % 4] = jnp.max(part, axis=0, keepdims=True)

        def soften(head):
            prob = jnp.exp2((scores[head % 4] - peaks[head % 4]) * scale)
            totals[head % 4] = jnp.sum(prob, axis=0, keepdims=True)
            probs[head % 4] = prob.astype(BF)

        def mix(head):
            part = jnp.dot(v_t[pl.ds(head * head_dim, head_dim), :], probs[head % 4], preferred_element_type=F32)
            mixed_t[pl.ds(head * head_dim, head_dim), :] = part * (1.0 / totals[head % 4])

        make_rows(0, bias_q, q_t, 0)
        make_keys(0)
        make_rows(2, bias_v, v_t, 0)
        for step in range(0, heads + 4, 2):
            for head in (step, step + 1):
                if head < heads:
                    score(head)
            ahead = step // group_heads + 1
            if ahead * group < width:
                if step % group_heads == 0:
                    make_rows(0, bias_q, q_t, ahead)
                    make_keys(ahead)
                else:
                    make_rows(2, bias_v, v_t, ahead)
            for head in (step - 2, step - 1):
                if 0 <= head < heads:
                    soften(head)
            for head in (step - 4, step - 3):
                if 0 <= head < heads:
                    mix(head)
            if step >= 4:
                cols = pl.ds((step - 4) * head_dim, 2 * head_dim)
                mixed[:, cols] = mixed_t[cols, :].T.astype(BF)

        for start in range(0, width, 512):
            cols = pl.ds(start, 512)
            part = jnp.dot(mixed[...], wout[layer, :, cols], preferred_element_type=F32) + bout[row, cols]
            state[:, cols] = (state[:, cols].astype(F32) + part).astype(BF)

        @when(image == 0)
        def _():
            for copy in weight_copies(layer)[2:]:
                copy.wait()

        @when(step_idx == 0)
        def _():
            for other in range(1, images):
                send_in(other, False)

        slot = me * images + image

        def give(peer):
            rows = pl.ds(peer * block, block) if isinstance(peer, int) else pl.ds(pl.multiple_of(peer * block, block), block)
            pltpu.make_async_remote_copy(
                src_ref=hid.at[image, rows, :], dst_ref=out_ref.at[slot],
                send_sem=out_send, recv_sem=out_recv,
                device_id={'sp': peer}, device_id_type=MESH).start()

        def leave():
            for peer in (1, 0):
                @pl.when(peer != me)
                def _():
                    give(peer)

            for hop in sorted(range(peers // 2), key=lambda hop: (-min(hop, peers // 2 - hop), hop)):
                for core in range(2):
                    peer = 2 * lax.rem(me // 2 + hop, peers // 2) + core

                    @pl.when(jnp.logical_and(peer != me, peer > 1))
                    def _():
                        give(peer)

            out_ref[slot] = hid[image, my_rows, :]

        chip_rows = 2 * block
        chips = peers // 2
        early = tuple(range(chips // 2 - 1)) + (chips - 2,)
        parts = (early, (chips // 2 - 1,) + tuple(chip for chip in reversed(range(chips)) if chip not in early + (chips // 2 - 1,)))

        def leave_part(part):
            for chip in parts[part]:
                for core in (1, 0):
                    peer = 2 * chip + core

                    @pl.when(peer != me)
                    def _():
                        give(peer)

                    @pl.when(peer == me)
                    def _():
                        out_ref[slot] = hid[image, my_rows, :]

        if last:
            half = tokens // 2

            def norm_part(part):
                for index, chip in enumerate(parts[part]):
                    norm_rows(state.at[pl.ds(chip * chip_rows, chip_rows), :],
                              normed.at[pl.ds(part * half + index * chip_rows, chip_rows), :], g2[row, :], s2[row, :], 32)

            def widen_part(part):
                rows = pl.ds(part * half, half)
                for start in range(0, mlp_dim, 512):
                    cols = pl.ds(start, 512)
                    part_up = jnp.dot(normed[rows, :], wup[layer, :, cols], preferred_element_type=F32) + bup[row, cols]
                    active[rows, cols] = gelu(part_up).astype(BF)

            def narrow_part(part):
                for start in range(0, width, 512):
                    cols = pl.ds(start, 512)
                    part_down = jnp.dot(active[pl.ds(part * half, half), :], wdown[layer, :, cols], preferred_element_type=F32) + bdown[row, cols]
                    for index, chip in enumerate(parts[part]):
                        rows = pl.ds(chip * chip_rows, chip_rows)
                        state[rows, cols] = (state[rows, cols].astype(F32) + part_down[index * chip_rows:(index + 1) * chip_rows]).astype(BF)

            norm_part(0)
            widen_part(0)
            norm_part(1)
            narrow_part(0)
            leave_part(0)
            widen_part(1)
            narrow_part(1)
            leave_part(1)
        else:
            norm_rows(state, normed, g2[row, :], s2[row, :], 32)
            for start in range(0, mlp_dim, 512):
                cols = pl.ds(start, 512)
                part = jnp.dot(normed[...], wup[layer, :, cols], preferred_element_type=F32) + bup[row, cols]
                active[:, cols] = gelu(part).astype(BF)
            for start in range(0, width, 512):
                cols = pl.ds(start, 512)
                part = jnp.dot(active[...], wdown[layer, :, cols], preferred_element_type=F32) + bdown[row, cols]
                state[:, cols] = (state[:, cols].astype(F32) + part).astype(BF)

            pl.when(layer == layers - 1)(leave)

    @pl.loop(0, images * layers - 1)
    def _(step_idx):
        body(step_idx)

    body(images * layers - 1)

    sent = x_ref.at[pl.ds(0, (peers - 1) * images)]
    pltpu.make_async_copy(sent, sent, in_send).wait()
    pltpu.make_async_copy(sent, sent, out_send).wait()
    pltpu.make_async_copy(sent, sent, out_recv).wait()


def solution(mesh):
    token_spec = P('dp', 'sp', None)
    peers = mesh.shape['sp']

    def device_step(image_tokens, ln1_gain, ln1_shift, w_qkv, b_qkv, w_out, b_out, ln2_gain, ln2_shift, w_up, b_up, w_down, b_down):
        total_images, block, width = image_tokens.shape
        layers, _, _, heads, head_dim = w_qkv.shape
        mlp_dim = w_up.shape[-1]
        images = total_images // peers
        tokens = block * peers
        inner = heads * head_dim
        w_qkv_t = jnp.transpose(w_qkv, (0, 2, 3, 4, 1)).reshape(layers, 3 * inner, width)
        w_out_m = w_out.reshape(layers, inner, width)
        args = (image_tokens, ln1_gain, ln1_shift, w_qkv_t, b_qkv, w_out_m, b_out, ln2_gain, ln2_shift, w_up, b_up, w_down, b_down)
        small = lambda a: pltpu.VMEM(a.shape, a.dtype)
        return pl.pallas_call(
            functools.partial(kernel, peers),
            out_shape=pltpu.VMEM(image_tokens.shape, image_tokens.dtype),
            in_specs=[pl.BlockSpec(memory_space=pl.ANY)] * len(args),
            out_specs=pl.BlockSpec(memory_space=pltpu.VMEM),
            scratch_shapes=[
                pltpu.VMEM((images, tokens, width), BF),
                small(w_qkv_t), small(w_out_m), small(w_up), small(w_down),
                small(ln1_gain), small(ln1_shift), small(b_qkv), small(b_out), small(ln2_gain), small(ln2_shift), small(b_up), small(b_down),
                pltpu.VMEM((tokens, width), BF),
                pltpu.VMEM((inner, tokens), BF),
                pltpu.VMEM((inner, tokens), BF),
                pltpu.VMEM((tokens, inner), BF),
                pltpu.VMEM((tokens, inner), BF),
                pltpu.VMEM((tokens, mlp_dim), BF),
                pltpu.VMEM((4, tokens, tokens), F32),
                pltpu.VMEM((4, tokens, tokens), BF),
                pltpu.VMEM((4, 1, tokens), F32),
                pltpu.VMEM((4, 1, tokens), F32),
                pltpu.VMEM((inner, tokens), F32),
                pltpu.SemaphoreType.REGULAR((peers,)),
                pltpu.SemaphoreType.DMA((layers, 4)),
                pltpu.SemaphoreType.DMA((8,)),
                pltpu.SemaphoreType.DMA,
                pltpu.SemaphoreType.DMA((images,)),
                pltpu.SemaphoreType.DMA,
                pltpu.SemaphoreType.DMA,
            ],
            compiler_params=pltpu.CompilerParams(collective_id=0, has_side_effects=True, vmem_limit_bytes=65_500_000),
        )(*args)

    return jax.shard_map(device_step, mesh=mesh, in_specs=(token_spec,) + (P(),) * 12, out_specs=token_spec, check_vma=False)
```
